32 devices in a mesh: seq: 8 (over z, x), head: 4 (over y, core).
Axes of the slice: x: 2, y: 2, z: 4, core: 2. Of those that a mesh axis runs over, the one named last changes fastest.
Arguments:
- hidden: bfloat16 [2048, 4096], P(('seq', 'head')), may hold values from -90 to 90
- block_order: int32 [16], replicated, may hold values from 0 to 15, as said below
- segment_ids: int32 [2048], replicated, may hold values from 0 to 3, never falling along the last dimension, each value on 1 to 1024 neighbouring positions
- w_query: bfloat16 [4096, 4096], P(None, 'head'), may hold values from -0.09375 to 0.09375
- key_weight: bfloat16 [4096, 1024], P(None, 'head'), may hold values from -0.09375 to 0.09375
- value_weight: bfloat16 [4096, 1024], P(None, 'head'), may hold values from -0.09375 to 0.09375
- w_out: bfloat16 [4096, 4096], P('head'), may hold values from -0.09375 to 0.09375
Outputs:
- layer_out: bfloat16 [2048, 4096], P(('seq', 'head'))
The draws below stay inside these ranges and needn't reach their ends.
Inputs may be any that keep to these rules, and one draw needn't show every extreme that they name: `block_order`: for each d, entries 2d and 2d+1 are two block numbers that sum to 15; every block number occurs once.
All inputs are finite; a program needn't handle non-finite values.
Results may differ from the reference program's by a relative error of at most 0.018.
The reference program's roundings to bfloat16 on the way (of `attended`) count: a program that leaves them out, or rounds other values in their place, can miss the bound.
Values may be sent and summed in bfloat16 or wider, within the bound.
A program may use at most 64 MiB of HBM per device.

```python
import math
import jax
import jax.numpy as jnp
import numpy as np
from jax import lax

MODEL_WIDTH = 4096
QUERY_HEADS = 32
KEY_VALUE_HEADS = 8
HEAD_SIZE = 128
TOKENS = 2048
BLK = 128
NBLK = 16
N_HEAD = 4


def draw_hidden(key, part):
    first_key = jax.random.fold_in(key, 0)
    return jnp.clip(jax.random.normal(first_key, (TOKENS, MODEL_WIDTH), jnp.float32), -6.0, 6.0).astype(jnp.bfloat16)


def draw_block_order(key, part):
    first_key, second_key = jax.random.split(jax.random.fold_in(key, 7))
    pairs = NBLK // 2
    shuffled = jax.random.permutation(first_key, pairs).astype(jnp.int32)
    flipped = jax.random.randint(second_key, (pairs,), 0, 2)
    earlier = jnp.where(flipped == 1, shuffled, NBLK - 1 - shuffled)
    later = NBLK - 1 - earlier
    return jnp.stack([earlier, later], axis=1).reshape(NBLK).astype(jnp.int32)


def steps_of(rng, shape, cuts, low, top_value):
    def one(axis_at, shards_of):
        draws = jax.random.uniform(jax.random.fold_in(jax.random.fold_in(rng, 6), axis_at), (shards_of,), jnp.float32, low / len(cuts), top_value / len(cuts))
        return jnp.repeat(jnp.exp(draws), shape[axis_at] // shards_of).reshape((-1,) + (1,) * (len(shape) - axis_at - 1))

    gain = one(*cuts[0])
    for cut in cuts[1:]:
        gain = gain * one(*cut)
    return gain


def length_profile(amount, total, most, slope):
    weights = [(1 << 20) // math.isqrt(rank ** slope) + 1 for rank in range(2, amount + 1)]
    surplus, given = total - most - (amount - 1), [1] * (amount - 1)
    while surplus > 0:
        free = [i for i in range(amount - 1) if given[i] < most]
        pool, left = sum([weights[i] for i in free]), surplus
        for i in free:
            addition = min(most - given[i], max(1, left * weights[i] // pool), surplus)
            given[i] = given[i] + addition
            surplus = surplus - addition
    return np.array([most] + given)


def ragged(own_key, amount, total, limit, slope):
    if amount == 2:
        one = jax.random.randint(own_key, (), max(1, total - limit), min(limit, total - 1) + 1)
        return jnp.stack([one, total - one])
    tallies = jnp.asarray(length_profile(amount, total, limit, slope), jnp.int32)
    pairs = (amount - 1) // 2
    source_of, receiver = tallies[1:1 + 2 * pairs:2], tallies[2:2 + 2 * pairs:2]
    margin = jnp.minimum(source_of - 1, limit - receiver)
    passed = jax.random.randint(jax.random.fold_in(own_key, 1), (pairs,), 0, 1 << 20) % (margin + 1)
    tallies = tallies.at[1:1 + 2 * pairs:2].set(source_of - passed).at[2:2 + 2 * pairs:2].set(receiver + passed)
    return tallies[jax.random.permutation(jax.random.fold_in(own_key, 2), amount)]


def centred(rng, dims, deviation, bound, cuts=(), held_as=jnp.bfloat16):
    values = jax.random.normal(rng, dims, jnp.float32) * deviation
    if len(cuts) > 0:
        values = steps_of(rng, dims, cuts, -0.22, 0.18) * values
    return jnp.clip(values, min=-bound, max=bound).astype(held_as)


def setup_inputs(seed: int = 0) -> dict:
    splits = jax.random.split(jax.random.key(seed), 8)
    hidden = draw_hidden(jax.random.fold_in(splits[7], 71), 0)
    block_order = draw_block_order(jax.random.fold_in(splits[7], 71), 0)
    segment_ids = jnp.searchsorted(jnp.cumsum(ragged(splits[2], 4, TOKENS, TOKENS // 2, 0)), jnp.arange(TOKENS), side="right").astype(jnp.int32)
    w_query = centred(splits[3], (MODEL_WIDTH, QUERY_HEADS * HEAD_SIZE), MODEL_WIDTH ** -0.5, 0.09375, ((1, 4),))
    key_weight = centred(splits[4], (MODEL_WIDTH, KEY_VALUE_HEADS * HEAD_SIZE), MODEL_WIDTH ** -0.5, 0.09375, ((1, 4),))
    value_weight = centred(splits[5], (MODEL_WIDTH, KEY_VALUE_HEADS * HEAD_SIZE), MODEL_WIDTH ** -0.5, 0.09375, ((1, 4),))
    w_out = centred(splits[6], (QUERY_HEADS * HEAD_SIZE, MODEL_WIDTH), (QUERY_HEADS * HEAD_SIZE) ** -0.5, 0.09375, ((0, 4),))
    return {"hidden": hidden, "block_order": block_order, "segment_ids": segment_ids, "w_query": w_query, "key_weight": key_weight, "value_weight": value_weight, "w_out": w_out}


NEGATIVE_FILLER = -1e30
ROPE_BASE = 500000.0


def apply_rotary(values, block_places, heads):
    count_rows = values.shape[0]
    shaped = values.reshape(count_rows, heads, HEAD_SIZE)
    half_dim = HEAD_SIZE // 2
    freqs = ROPE_BASE ** (-(jnp.arange(half_dim, dtype=jnp.float32) * 2.0 / HEAD_SIZE))
    angles = block_places.astype(jnp.float32)[:, None] * freqs[None, :]
    cosine = jnp.cos(angles)[:, None, :]
    sine = jnp.sin(angles)[:, None, :]
    first_half = shaped[:, :, :half_dim]
    second_half = shaped[:, :, half_dim:]
    turned = jnp.concatenate([first_half * cosine - second_half * sine, second_half * cosine + first_half * sine], axis=2)
    return turned.reshape(count_rows, heads * HEAD_SIZE)


def attend(carry_state, query_matrix, query_pos, query_seg, key_block, value_block, key_pos, key_seg):
    running, totals, weighted = carry_state
    scores = jnp.einsum("qhgd,khd->hgqk", query_matrix.astype(jnp.float32), key_block.astype(jnp.float32)) * (HEAD_SIZE ** -0.5)
    allowed = (key_pos[None, :] <= query_pos[:, None]) & (key_seg[None, :] == query_seg[:, None])
    masked = jnp.where(allowed, scores, NEGATIVE_FILLER)
    newmax = jnp.maximum(running, jnp.max(masked, axis=3))
    expo = jnp.where(allowed, jnp.exp(scores - newmax[..., None]), 0.0)
    factor = jnp.exp(running - newmax)
    totals = totals * factor + jnp.sum(expo, axis=3)
    rounded = expo.astype(jnp.bfloat16).astype(jnp.float32)
    weighted = weighted * factor[..., None] + jnp.einsum("hgqk,khd->hgqd", rounded, value_block.astype(jnp.float32))
    return newmax, totals, weighted


def reference(hidden, block_order, segment_ids, w_query, key_weight, value_weight, w_out):
    inverse = jnp.zeros((NBLK,), jnp.int32).at[block_order].set(jnp.arange(NBLK, dtype=jnp.int32))
    sorted_blocks = hidden.reshape(NBLK, BLK, MODEL_WIDTH)[inverse].reshape(TOKENS, MODEL_WIDTH)
    block_places = jnp.arange(TOKENS, dtype=jnp.int32)
    query_matrix = apply_rotary(jnp.dot(sorted_blocks, w_query, preferred_element_type=jnp.float32), block_places, QUERY_HEADS).astype(jnp.bfloat16)
    every_key = apply_rotary(jnp.dot(sorted_blocks, key_weight, preferred_element_type=jnp.float32), block_places, KEY_VALUE_HEADS).astype(jnp.bfloat16)
    every_value = jnp.dot(sorted_blocks, value_weight, preferred_element_type=jnp.float32).astype(jnp.bfloat16)
    query_group = QUERY_HEADS // KEY_VALUE_HEADS
    query_block = math.gcd(512, TOKENS)
    nblocks = TOKENS // query_block

    def outer(index, outputs):
        starting_row = (index * query_block).astype(jnp.int32)
        query_rows = lax.dynamic_slice_in_dim(query_matrix, starting_row, query_block, 0).reshape(query_block, KEY_VALUE_HEADS, query_group, HEAD_SIZE)
        qpos = starting_row + jnp.arange(query_block, dtype=jnp.int32)
        qseg = lax.dynamic_slice_in_dim(segment_ids, starting_row, query_block, 0)
        start_state = (jnp.full((KEY_VALUE_HEADS, query_group, query_block), NEGATIVE_FILLER, jnp.float32),
                   jnp.zeros((KEY_VALUE_HEADS, query_group, query_block), jnp.float32),
                   jnp.zeros((KEY_VALUE_HEADS, query_group, query_block, HEAD_SIZE), jnp.float32))

        def inner_loop(key_index, carry_state):
            leading_key = (key_index * query_block).astype(jnp.int32)
            key_block = lax.dynamic_slice_in_dim(every_key, leading_key, query_block, 0).reshape(query_block, KEY_VALUE_HEADS, HEAD_SIZE)
            value_block = lax.dynamic_slice_in_dim(every_value, leading_key, query_block, 0).reshape(query_block, KEY_VALUE_HEADS, HEAD_SIZE)
            key_pos = leading_key + jnp.arange(query_block, dtype=jnp.int32)
            key_seg = lax.dynamic_slice_in_dim(segment_ids, leading_key, query_block, 0)
            return attend(carry_state, query_rows, qpos, qseg, key_block, value_block, key_pos, key_seg)

        finished = lax.fori_loop(0, index + 1, inner_loop, start_state)
        block_out = (finished[2] / finished[1][..., None]).transpose(2, 0, 1, 3).reshape(query_block, QUERY_HEADS * HEAD_SIZE)
        return lax.dynamic_update_slice_in_dim(outputs, block_out.astype(jnp.bfloat16), starting_row, 0)

    attended = lax.fori_loop(0, nblocks, outer, jnp.zeros((TOKENS, QUERY_HEADS * HEAD_SIZE), jnp.bfloat16))
    width = QUERY_HEADS * HEAD_SIZE // N_HEAD
    summed = jnp.zeros((TOKENS, MODEL_WIDTH), jnp.float32)
    for member in range(N_HEAD):
        partial_sum = jnp.dot(attended[:, member * width:(member + 1) * width], w_out[member * width:(member + 1) * width], preferred_element_type=jnp.float32)
        summed = summed + partial_sum.astype(jnp.bfloat16).astype(jnp.float32)
    result = summed.astype(jnp.bfloat16).reshape(NBLK, BLK, MODEL_WIDTH)[block_order].reshape(TOKENS, MODEL_WIDTH)
    return result
```

```python
import functools
import math

import jax
import jax.numpy as jnp
import numpy as np
from jax import lax
from jax.experimental import pallas as pl
from jax.experimental.pallas import tpu as pltpu
from jax.sharding import PartitionSpec as P

HEAD_SIZE = 128
NEGATIVE_FILLER = -1e30
ROPE_BASE = 500000.0
DOCS = 4
CORES = 2
LAG = 3
MESH = pl.DeviceIdType.MESH
F32 = jnp.float32
BF16 = jnp.bfloat16


def rotated(t, cosine, sine):
    heads = t.shape[1] // HEAD_SIZE
    pieces = []
    for h in range(heads):
        one = t[:, h * HEAD_SIZE:(h + 1) * HEAD_SIZE]
        pieces.append(one * cosine + pltpu.roll(one, HEAD_SIZE // 2, 1) * sine)
    return pieces


def kernel(
    X, Z, Y, NO, NP,
    order, hidden, seg_hbm, freq_hbm, wq, wk, wv, wo_hbm, out,
    seg, freq, xg, wb, wo, acc, cos_t, sin_t, kv, att, keep, give, rb, sb, fb, *rest,
):
    far_side, near_side = rest[:6], rest[6:12]
    (in_sem, hn_sem, wkv_sem, wq_sem, wo_sem, hs_sem, hp_sem, hd_sem, hr_sem,
     xs_sem, zs_sem, kc_sem, kx_sem, ps_sem, pf_sem, pn_sem, ys_sem, yr_sem) = rest[12:]
    r, D = hidden.shape
    R = xg.shape[0]
    Cq, Ck = wq.shape[1], wk.shape[1]
    half = R // 2
    q_heads, kv_heads = Cq // HEAD_SIZE, Ck // HEAD_SIZE
    group = q_heads // kv_heads
    W = Cq + 2 * Ck
    near_rows, far_rows = CORES * r, R - CORES * r
    part = r // 2
    s_id, h_id = lax.axis_index("seq"), lax.axis_index("head")
    y, c = h_id // CORES, h_id % CORES
    z, x = s_id // X, s_id % X
    partner = y * CORES + (1 - c)

    def peer_y(j):
        return lax.rem(y + j, Y)

    def far_at(j, e):
        return near_rows + e * (Y - 1) * r + (j - 1) * r

    runs = [(0, r, h_id * r), (r, r, partner * r)]
    for e in range(2):
        for j in range(1, Y):
            for i, core in enumerate((c, 1 - c)):
                runs.append((far_at(j, e) + i * part, part, (peer_y(j) * CORES + core) * r + e * part))
    pieces = [(0, r), (r, r), (near_rows, (Y - 1) * r), (near_rows + (Y - 1) * r, (Y - 1) * r)]
    units = [(0, near_rows), (near_rows, far_rows)]

    def place(slot, first):
        return order[2 * slot + first // half] * half + lax.rem(first, half)

    barrier = pltpu.get_barrier_semaphore()

    def greet(sq, hd):
        pl.semaphore_signal(barrier, inc=1, device_id=(sq, hd), device_id_type=MESH)

    greet(s_id, partner)
    for j in range(1, Y):
        greet(s_id, peer_y(j) * CORES + c)
    for k in range(1, X):
        greet(z * X + lax.rem(x + k, X), h_id)

    for d in range(1, Z):
        greet(lax.rem(z + d, Z) * X + x, h_id)

    own_rows = pltpu.make_async_copy(hidden, xg.at[pl.ds(0, r), :], hn_sem)
    own_rows.start()
    seg_copy = pltpu.make_async_copy(seg_hbm, seg, in_sem.at[0])
    freq_copy = pltpu.make_async_copy(freq_hbm, freq, in_sem.at[1])
    freq_copy.start()
    seg_copy.start()
    wk_copy = pltpu.make_async_copy(wk, wb.at[:, pl.ds(Cq, Ck)], wkv_sem.at[0])
    wv_copy = pltpu.make_async_copy(wv, wb.at[:, pl.ds(Cq + Ck, Ck)], wkv_sem.at[1])
    wq_copy = pltpu.make_async_copy(wq, wb.at[:, pl.ds(0, Cq)], wq_sem)
    wo_copy = pltpu.make_async_copy(wo_hbm, wo, wo_sem)
    wk_copy.start()
    wv_copy.start()

    pl.semaphore_wait(barrier, 1 + (Y - 1) + (X - 1) + (Z - 1))

    def hid_pair():
        return pltpu.make_async_remote_copy(
            src_ref=xg.at[pl.ds(0, r), :], dst_ref=xg.at[pl.ds(r, r), :],
            send_sem=hs_sem, recv_sem=hp_sem,
            device_id=(s_id, partner), device_id_type=MESH,
        )

    def hid_send(j, e):
        return pltpu.make_async_remote_copy(
            src_ref=xg.at[pl.ds(e * part, part), :], dst_ref=xg.at[pl.ds(far_at(Y - j, e), part), :],
            send_sem=hs_sem, recv_sem=hd_sem.at[Y - j - 1, e],
            device_id=(s_id, peer_y(j) * CORES + c), device_id_type=MESH,
        )

    def hid_direct(j, e):
        rows = xg.at[pl.ds(far_at(j, e), part), :]
        return pltpu.make_async_remote_copy(
            src_ref=rows, dst_ref=rows, send_sem=hs_sem, recv_sem=hd_sem.at[j - 1, e],
            device_id=(s_id, partner), device_id_type=MESH,
        )

    def hid_relay(j, e):
        return pltpu.make_async_remote_copy(
            src_ref=xg.at[pl.ds(far_at(j, e), part), :],
            dst_ref=xg.at[pl.ds(far_at(j, e) + part, part), :],
            send_sem=hs_sem, recv_sem=hr_sem.at[j - 1, e],
            device_id=(s_id, partner), device_id_type=MESH,
        )

    own_rows.wait()
    hid_pair().start()
    for e in range(2):
        for j in range(1, Y):
            hid_send(j, e).start()
    wq_copy.start()

    freq_copy.wait()
    for lo, n, first in runs:
        lane = lax.broadcasted_iota(jnp.int32, (n, HEAD_SIZE), 1)
        row = lax.broadcasted_iota(jnp.int32, (n, HEAD_SIZE), 0)
        angle = (row + place(s_id, first)).astype(F32) * freq[...]
        cos_t[lo:lo + n, :] = jnp.cos(angle)
        sn = jnp.sin(angle)
        sin_t[lo:lo + n, :] = jnp.where(lane < HEAD_SIZE // 2, -sn, sn)

    def kv_rows(zb, xb, lo, n):
        return kv.at[pl.ds((zb * X + xb) * R + lo, n), :]

    def col_copy(zb, p, target, sem):
        rows = kv_rows(zb, x, *pieces[p])
        return pltpu.make_async_remote_copy(
            src_ref=rows, dst_ref=rows, send_sem=sem, recv_sem=kc_sem.at[zb, p],
            device_id=(target, h_id), device_id_type=MESH,
        )

    def cross_copy(zb, xb, p, way, target, sem):
        rows = kv_rows(zb, xb, *pieces[p])
        return pltpu.make_async_remote_copy(
            src_ref=rows, dst_ref=rows, send_sem=sem, recv_sem=kx_sem.at[way - 1, zb, p],
            device_id=(target, h_id), device_id_type=MESH,
        )

    def send_x(zb, p):
        for k in range(1, X):
            cross_copy(zb, x, p, X - k, z * X + lax.rem(x + k, X), xs_sem).start()

    def send_up(zb, p):
        @pl.when(z < Z - 1)
        def _():
            col_copy(zb, p, s_id + X, zs_sem).start()

    def send_down(zb, p):
        @pl.when(z > 0)
        def _():
            col_copy(zb, p, s_id - X, zs_sem).start()

    def send_own(p):
        if p < 2:
            send_up(z, p)
            send_down(z, p)
        else:
            for d in range(Z - 1, 0, -1):
                @pl.when(z + d < Z)
                def _(d=d):
                    col_copy(z, p, s_id + d * X, zs_sem).start()

                @pl.when(z - d >= 0)
                def _(d=d):
                    col_copy(z, p, s_id - d * X, zs_sem).start()
        send_x(z, p)

    def pass_on(d, p):
        @pl.when(z - d >= 0)
        def _():
            col_copy(z - d, p, s_id, zs_sem).wait_recv()
            if p < 2:
                send_up(z - d, p)
            if d > 1 or p < 2:
                send_x(z - d, p)

        @pl.when(z + d < Z)
        def _():
            col_copy(z + d, p, s_id, zs_sem).wait_recv()
            if p < 2:
                send_down(z + d, p)
            if d > 1 or p < 2:
                send_x(z + d, p)

    def cross_wait(zb, way, p):
        cross_copy(zb, lax.rem(x + way, X), p, way, s_id, xs_sem).wait_recv()

    def cross_on(way, p):
        xb = lax.rem(x + way, X)
        cross_wait(z, way, p)

        @pl.when(z < Z - 1)
        def _():
            cross_copy(z, xb, p, way, s_id + X, zs_sem).start()

        @pl.when(z > 0)
        def _():
            cross_copy(z, xb, p, way, s_id - X, zs_sem).start()

    def store_kv(p):
        lo, n = pieces[p]
        got = jnp.dot(xg[lo:lo + n, :], wb[:, Cq:W], preferred_element_type=F32)
        turned = rotated(got[:, :Ck], cos_t[lo:lo + n, :], sin_t[lo:lo + n, :])
        rows = pl.ds(s_id * R + lo, n)
        for h in range(kv_heads):
            kv[rows, h * HEAD_SIZE:(h + 1) * HEAD_SIZE] = turned[h].astype(BF16)
        kv[rows, Ck:2 * Ck] = got[:, Ck:].astype(BF16)
        send_own(p)

    def store_q(u, side):
        lo, n = units[u]
        q = side[0]
        acc[0:n, :] = jnp.dot(xg[lo:lo + n, :], wb[:, :Cq], preferred_element_type=F32)
        turned = rotated(acc[0:n, :], cos_t[lo:lo + n, :], sin_t[lo:lo + n, :])
        for h in range(q_heads):
            at = (h % group) * n
            q[h // group, at:at + n, :] = turned[h].astype(BF16)

    wk_copy.wait()
    wv_copy.wait()
    store_kv(0)

    seg_copy.wait()
    starts = [
        jnp.sum(jnp.sum((seg[...] < v).astype(jnp.int32), axis=0, keepdims=True), axis=1, keepdims=True)
        for v in range(1, DOCS)
    ]
    for u, side in enumerate((near_side, far_side)):
        lo, n = units[u]
        info = side[5]
        for at, m, first in runs:
            if not lo <= at < lo + n:
                continue
            pos = lax.broadcasted_iota(jnp.int32, (1, m), 1) + place(s_id, first)
            start = jnp.zeros_like(pos)
            for begun in starts:
                start = jnp.where(begun <= pos, jnp.maximum(start, begun), start)
            for gh in range(info.shape[1] // n):
                lanes = slice(gh * n + at - lo, gh * n + at - lo + m)
                info[0:1, lanes] = pos
                info[1:2, lanes] = start
    for side in (far_side, near_side):
        side[1][...] = jnp.full_like(side[1], NEGATIVE_FILLER)
        side[2][...] = jnp.zeros_like(side[2])
        side[3][...] = jnp.zeros_like(side[3])

    hid_pair().wait_recv()
    store_kv(1)
    wo_copy.start()
    wq_copy.wait()
    store_q(0, near_side)

    scale = math.log2(math.e) / math.sqrt(HEAD_SIZE)
    nt = (((1,), (1,)), ((), ()))

    def attend(slot, u, side):
        q, m_s, l_s, o_s, bias, info = side
        chunk = bias.shape[1]
        lo, n = units[u]
        for at, m, first in runs:
            if not lo <= at < lo + n:
                continue
            kpos = lax.broadcasted_iota(jnp.int32, (m, chunk), 0) + place(slot, first)
            ok = (kpos <= info[0:1, :]) & (kpos >= info[1:2, :])
            bias[at - lo:at - lo + m, :] = jnp.where(ok, 0.0, NEGATIVE_FILLER)
        work = [(kh, w) for kh in range(kv_heads) for w in range(q.shape[1] // chunk)]
        span = lambda w: slice(w * chunk, (w + 1) * chunk)
        rows = pl.ds(slot * R + lo, n)
        keys = [kv[rows, kh * HEAD_SIZE:(kh + 1) * HEAD_SIZE] for kh in range(kv_heads)]
        vals = [
            kv[rows, Ck + kh * HEAD_SIZE:Ck + (kh + 1) * HEAD_SIZE].T for kh in range(kv_heads)
        ]

        def scores(item):
            kh, w = item
            return lax.dot_general(keys[kh], q[kh, span(w), :], nt, preferred_element_type=F32)

        ahead = scores(work[0])
        for i, (kh, w) in enumerate(work):
            raw = ahead
            if i + 1 < len(work):
                ahead = scores(work[i + 1])
            cols = span(w)
            s = raw * scale + bias[0:n, :]
            old = m_s[kh:kh + 1, cols]
            new = jnp.maximum(old, jnp.max(s, axis=0, keepdims=True))
            p = jnp.exp2(s - new)
            alpha = jnp.exp2(old - new)
            m_s[kh:kh + 1, cols] = new
            l_s[kh:kh + 1, cols] = l_s[kh:kh + 1, cols] * alpha + jnp.sum(p, axis=0, keepdims=True)
            o_s[kh, :, cols] = o_s[kh, :, cols] * alpha + jnp.dot(
                vals[kh], p.astype(BF16), preferred_element_type=F32
            )

    def visit(u, side, first, last, ways, wait):
        A, B = ways

        def one(i, _):
            d, rest_i = i // (2 * (B - A)), lax.rem(i, 2 * (B - A))
            sign, way = rest_i // (B - A), A + lax.rem(rest_i, B - A)
            zb = jnp.where(sign == 0, z - d, z + d)

            @pl.when((zb >= 0) & (zb < Z) & ((d > 0) | (sign == 0)))
            def _():
                if wait:
                    for p in wait:
                        cross_wait(zb, way, p)
                attend(zb * X + lax.rem(x + way, X), u, side)

            return 0

        lax.fori_loop(first * 2 * (B - A), last * 2 * (B - A), one, 0)

    def settle(side, lo):
        q, m_s, l_s, o_s, bias, info = side
        wide = q.shape[1] // group
        for h in range(q_heads):
            kh, gh = h // group, h % group
            lanes = slice(gh * wide, (gh + 1) * wide)
            att[lo:lo + wide, h * HEAD_SIZE:(h + 1) * HEAD_SIZE] = (
                o_s[kh, :, lanes] / l_s[kh:kh + 1, lanes]
            ).T.astype(BF16)

    column, others = (0, 1), (1, X)


    def relay(first, last, p):
        for d in range(first, min(last, Z)):
            pass_on(d, p)

    def hidden_on(e):
        for j in range(1, Y):
            hid_direct(j, e).wait_recv()
            hid_relay(j, e).start()

    def hidden_in(e):
        for j in range(1, Y):
            hid_relay(j, e).wait_recv()

    N_BOTH, F_BOTH = (0, 1), (2, 3)

    relay(1, 2, 0)
    visit(0, near_side, 0, 1, column, ())
    relay(1, 2, 1)
    visit(0, near_side, 1, min(2, Z), column, ())
    hidden_on(0)
    hidden_in(0)
    store_kv(2)
    relay(2, 3, 0)
    relay(2, 3, 1)
    visit(0, near_side, 0, 1, others, N_BOTH)
    visit(0, near_side, 2, min(3, Z), column, ())
    visit(0, near_side, 1, min(2, Z), others, N_BOTH)
    hidden_on(1)
    hidden_in(1)
    store_kv(3)
    for way in range(1, X):
        cross_on(way, 2)
    store_q(1, far_side)
    relay(3, Z, 0)
    relay(3, Z, 1)
    visit(0, far_side, 0, min(2, Z), (0, X), ())
    relay(1, Z, 2)
    for way in range(1, X):
        cross_on(way, 3)
    visit(0, far_side, 2, Z, column, ())
    relay(1, Z, 3)
    visit(0, far_side, 2, Z, others, N_BOTH)
    visit(1, far_side, 0, Z, column, ())
    visit(1, far_side, 0, 1, others, ())
    visit(1, far_side, 1, Z, others, F_BOTH)
    settle(far_side, near_rows)
    wo_copy.wait()

    NW, PW = D // NO, D // NP

    def pair_far(j, n):
        cols = pl.ds(n * NW, NW)
        return pltpu.make_async_remote_copy(
            src_ref=give.at[j, :, cols], dst_ref=rb.at[j, :, cols],
            send_sem=ps_sem, recv_sem=pf_sem.at[j - 1, n],
            device_id=(s_id, partner), device_id_type=MESH,
        )

    def pair_near(n):
        cols = pl.ds(n * PW, PW)
        return pltpu.make_async_remote_copy(
            src_ref=give.at[0, :, cols], dst_ref=rb.at[0, :, cols],
            send_sem=ps_sem, recv_sem=pn_sem.at[n],
            device_id=(s_id, partner), device_id_type=MESH,
        )

    def far_copy(j, n):
        cols = pl.ds(n * NW, NW)
        return pltpu.make_async_remote_copy(
            src_ref=sb.at[j - 1, :, cols], dst_ref=fb.at[j - 1, :, cols],
            send_sem=ys_sem, recv_sem=yr_sem.at[j - 1, n],
            device_id=(s_id, peer_y(j) * CORES + c), device_id_type=MESH,
        )

    def project_far(n, _):
        @pl.when(n < NO)
        def _():
            cols = pl.ds(n * NW, NW)
            got = jnp.dot(att[near_rows:R, :], wo[:, cols], preferred_element_type=F32).astype(BF16)
            for j in range(1, Y):
                for e in range(2):
                    at = far_at(j, e) - near_rows
                    keep[j, e * part:(e + 1) * part, cols] = got[at:at + part, :]
                    give[j, e * part:(e + 1) * part, cols] = got[at + part:at + r, :]
                pair_far(j, n).start()

        @pl.when(n >= LAG)
        def _():
            cols = pl.ds((n - LAG) * NW, NW)
            for j in range(1, Y):
                pair_far(j, n - LAG).wait_recv()
                sb[j - 1, :, cols] = (keep[j, :, cols].astype(F32) + rb[j, :, cols].astype(F32)).astype(BF16)
                far_copy(j, n - LAG).start()

        return 0

    lax.fori_loop(0, NO + LAG, project_far, 0)
    visit(0, near_side, 3, Z, column, ())
    visit(0, near_side, 2, Z, others, ())
    visit(1, near_side, 0, Z, (0, X), ())
    settle(near_side, 0)

    def project_near(n, _):
        cols = pl.ds(n * PW, PW)
        got = jnp.dot(att[0:near_rows, :], wo[:, cols], preferred_element_type=F32).astype(BF16)
        keep[0, :, cols] = got[:r, :]
        give[0, :, cols] = got[r:, :]
        pair_near(n).start()
        return 0

    lax.fori_loop(0, NP, project_near, 0)

    for n in range(NP):
        pair_near(n).wait_recv()

    def finish(n, _):
        cols = pl.ds(n * NW, NW)
        total = keep[0, :, cols].astype(F32) + rb[0, :, cols].astype(F32)
        for j in range(1, Y):
            far_copy(j, n).wait_recv()
            total = total + fb[j - 1, :, cols].astype(F32)
        out[:, cols] = total.astype(BF16)
        return 0

    lax.fori_loop(0, NO, finish, 0)

    def drain(ref, sem):
        pltpu.make_async_copy(ref, ref, sem).wait()

    drain(xg.at[pl.ds(0, (2 * Y - 1) * r), :], hs_sem)
    drain(give, ps_sem)
    drain(sb, ys_sem)
    for zz in range(Z):
        ups, downs = (zz + 1 if zz < Z - 1 else 0), (Z - zz if zz > 0 else 0)
        beside = (zz > 0) + (zz < Z - 1)
        along = (ups + downs) * near_rows + (Z - 1 + (X - 1) * beside) * far_rows
        over = (X - 1) * (Z * R - beside * far_rows)

        @pl.when(z == zz)
        def _(along=along, over=over):
            drain(kv.at[pl.ds(0, along), :], zs_sem)
            drain(kv.at[pl.ds(0, over), :], xs_sem)


def on_device(X, Z, Y, hidden, block_order, segment_ids, w_query, key_weight, value_weight, w_out):
    r, D = hidden.shape
    S, H = X * Z, Y * CORES
    R = r * H
    Cq, Ck = w_query.shape[1], key_weight.shape[1]
    W = Cq + 2 * Ck
    q_heads = Cq // HEAD_SIZE
    NO, NP = max(1, D // 512), max(1, D // 1024)
    exponent = np.arange(HEAD_SIZE // 2, dtype=np.float64) * 2.0 / HEAD_SIZE
    freqs = np.tile(ROPE_BASE ** (-exponent), 2).astype(np.float32)[None, :]
    dma = pltpu.SemaphoreType.DMA
    kv_heads = Ck // HEAD_SIZE
    group = q_heads // kv_heads
    near_rows, far_rows = CORES * r, R - CORES * r
    segments = segment_ids.reshape(block_order.shape[0], -1)

    def half_scratch(rows):
        together = 2 if rows % HEAD_SIZE == 0 and group % 2 == 0 else group
        lanes = group * rows
        return [
            pltpu.VMEM((kv_heads, lanes, HEAD_SIZE), BF16),
            pltpu.VMEM((kv_heads, lanes), F32),
            pltpu.VMEM((kv_heads, lanes), F32),
            pltpu.VMEM((kv_heads, HEAD_SIZE, lanes), F32),
            pltpu.VMEM((max(near_rows, far_rows), together * rows), F32),
            pltpu.VMEM((2, together * rows), jnp.int32),
        ]

    far = max(1, Y - 1)
    anywhere = pl.BlockSpec(memory_space=pl.ANY)
    return pl.pallas_call(
        functools.partial(kernel, X, Z, Y, NO, NP),
        out_shape=pltpu.VMEM((r, D), BF16),
        in_specs=[pl.BlockSpec(memory_space=pltpu.SMEM)] + [anywhere] * 7,
        out_specs=pl.BlockSpec(memory_space=pltpu.VMEM),
        scratch_shapes=[
            pltpu.VMEM(segments.shape, jnp.int32),
            pltpu.VMEM((1, HEAD_SIZE), F32),
            pltpu.VMEM((R, D), BF16),
            pltpu.VMEM((D, W), BF16),
            pltpu.VMEM((Cq, D), BF16),
            pltpu.VMEM((max(near_rows, far_rows), Cq), F32),
            pltpu.VMEM((R, HEAD_SIZE), F32),
            pltpu.VMEM((R, HEAD_SIZE), F32),
            pltpu.VMEM((S * R, 2 * Ck), BF16),
            pltpu.VMEM((R, Cq), BF16),
            pltpu.VMEM((Y, r, D), BF16),
            pltpu.VMEM((Y, r, D), BF16),
            pltpu.VMEM((Y, r, D), BF16),
            pltpu.VMEM((far, r, D), BF16),
            pltpu.VMEM((far, r, D), BF16),
            *half_scratch(far_rows),
            *half_scratch(near_rows),
            dma((2,)), dma, dma((2,)), dma, dma,
            dma, dma, dma((far, 2)), dma((far, 2)),
            dma, dma, dma((Z, 4)), dma((max(1, X - 1), Z, 4)),
            dma, dma((far, NO)), dma((NP,)), dma, dma((far, NO)),
        ],
        compiler_params=pltpu.CompilerParams(
            collective_id=0, has_side_effects=True, vmem_limit_bytes=60 * 1024 * 1024
        ),
    )(
        block_order, hidden, segments, jnp.asarray(freqs),
        w_query, key_weight, value_weight, w_out,
    )


def solution(mesh):
    seq, head = mesh.shape["seq"], mesh.shape["head"]
    X = 1
    while 4 * X * X <= seq and seq % (2 * X) == 0:
        X *= 2
    placed = (
        P(("seq", "head"), None),
        P(),
        P(),
        P(None, "head"),
        P(None, "head"),
        P(None, "head"),
        P("head", None),
    )
    return jax.shard_map(
        functools.partial(on_device, X, seq // X, head // CORES),
        mesh=mesh, in_specs=placed, out_specs=P(("seq", "head"), None), check_vma=False,
    )
```

```python
import functools
import math

import jax
import jax.numpy as jnp
import numpy as np
from jax import lax
from jax.experimental import pallas as pl
from jax.experimental.pallas import tpu as pltpu
from jax.sharding import PartitionSpec as P

HEAD_SIZE = 128
NEGATIVE_FILLER = -1e30
ROPE_BASE = 500000.0
DOCS = 4
CORES = 2
LAG = 3
MESH = pl.DeviceIdType.MESH
F32 = jnp.float32
BF16 = jnp.bfloat16


def rotated(t, cosine, sine):
    heads = t.shape[1] // HEAD_SIZE
    pieces = []
    for h in range(heads):
        one = t[:, h * HEAD_SIZE:(h + 1) * HEAD_SIZE]
        pieces.append(one * cosine + pltpu.roll(one, HEAD_SIZE // 2, 1) * sine)
    return pieces


def kernel(
    X, Z, Y, NO, NP,
    order, hidden, seg_hbm, freq_hbm, wq, wk, wv, wo_hbm, out,
    seg, freq, xg, wb, wo, acc, cos_t, sin_t, kv, att, keep, give, rb, sb, fb, *rest,
):
    far_side, near_side = rest[:6], rest[6:12]
    (in_sem, hn_sem, wkv_sem, wq_sem, wo_sem, hs_sem, hp_sem, hd_sem, hr_sem,
     xs_sem, zs_sem, kc_sem, kx_sem, ps_sem, pf_sem, pn_sem, ys_sem, yr_sem) = rest[12:]
    r, D = hidden.shape
    R = xg.shape[0]
    Cq, Ck = wq.shape[1], wk.shape[1]
    half = R // 2
    q_heads, kv_heads = Cq // HEAD_SIZE, Ck // HEAD_SIZE
    group = q_heads // kv_heads
    W = Cq + 2 * Ck
    near_rows, far_rows = CORES * r, R - CORES * r
    part = r // 2
    s_id, h_id = lax.axis_index("seq"), lax.axis_index("head")
    y, c = h_id // CORES, h_id % CORES
    z, x = s_id // X, s_id % X
    partner = y * CORES + (1 - c)

    def peer_y(j):
        return lax.rem(y + j, Y)

    def far_at(j, e):
        return near_rows + e * (Y - 1) * r + (j - 1) * r

    runs = [(0, r, h_id * r), (r, r, partner * r)]
    for e in range(2):
        for j in range(1, Y):
            for i, core in enumerate((c, 1 - c)):
                runs.append((far_at(j, e) + i * part, part, (peer_y(j) * CORES + core) * r + e * part))
    pieces = [(0, r), (r, r), (near_rows, (Y - 1) * r), (near_rows + (Y - 1) * r, (Y - 1) * r)]
    units = [(0, near_rows), (near_rows, far_rows)]

    def place(slot, first):
        return order[2 * slot + first // half] * half + lax.rem(first, half)

    barrier = pltpu.get_barrier_semaphore()

    def greet(sq, hd):
        pl.semaphore_signal(barrier, inc=1, device_id=(sq, hd), device_id_type=MESH)

    greet(s_id, partner)
    for j in range(1, Y):
        greet(s_id, peer_y(j) * CORES + c)
    for k in range(1, X):
        greet(z * X + lax.rem(x + k, X), h_id)

    @pl.when(z > 0)
    def _():
        greet(s_id - X, h_id)

    @pl.when(z < Z - 1)
    def _():
        greet(s_id + X, h_id)

    own_rows = pltpu.make_async_copy(hidden, xg.at[pl.ds(0, r), :], hn_sem)
    own_rows.start()
    seg_copy = pltpu.make_async_copy(seg_hbm, seg, in_sem.at[0])
    freq_copy = pltpu.make_async_copy(freq_hbm, freq, in_sem.at[1])
    freq_copy.start()
    seg_copy.start()
    wk_copy = pltpu.make_async_copy(wk, wb.at[:, pl.ds(Cq, Ck)], wkv_sem.at[0])
    wv_copy = pltpu.make_async_copy(wv, wb.at[:, pl.ds(Cq + Ck, Ck)], wkv_sem.at[1])
    wq_copy = pltpu.make_async_copy(wq, wb.at[:, pl.ds(0, Cq)], wq_sem)
    wo_copy = pltpu.make_async_copy(wo_hbm, wo, wo_sem)
    wk_copy.start()
    wv_copy.start()

    near = jnp.where(z > 0, 1, 0) + jnp.where(z < Z - 1, 1, 0)
    pl.semaphore_wait(barrier, 1 + (Y - 1) + (X - 1) + near)

    def hid_pair():
        return pltpu.make_async_remote_copy(
            src_ref=xg.at[pl.ds(0, r), :], dst_ref=xg.at[pl.ds(r, r), :],
            send_sem=hs_sem, recv_sem=hp_sem,
            device_id=(s_id, partner), device_id_type=MESH,
        )

    def hid_send(j, e):
        return pltpu.make_async_remote_copy(
            src_ref=xg.at[pl.ds(e * part, part), :], dst_ref=xg.at[pl.ds(far_at(Y - j, e), part), :],
            send_sem=hs_sem, recv_sem=hd_sem.at[Y - j - 1, e],
            device_id=(s_id, peer_y(j) * CORES + c), device_id_type=MESH,
        )

    def hid_direct(j, e):
        rows = xg.at[pl.ds(far_at(j, e), part), :]
        return pltpu.make_async_remote_copy(
            src_ref=rows, dst_ref=rows, send_sem=hs_sem, recv_sem=hd_sem.at[j - 1, e],
            device_id=(s_id, partner), device_id_type=MESH,
        )

    def hid_relay(j, e):
        return pltpu.make_async_remote_copy(
            src_ref=xg.at[pl.ds(far_at(j, e), part), :],
            dst_ref=xg.at[pl.ds(far_at(j, e) + part, part), :],
            send_sem=hs_sem, recv_sem=hr_sem.at[j - 1, e],
            device_id=(s_id, partner), device_id_type=MESH,
        )

    own_rows.wait()
    hid_pair().start()
    for e in range(2):
        for j in range(1, Y):
            hid_send(j, e).start()
    wq_copy.start()

    freq_copy.wait()
    for lo, n, first in runs:
        lane = lax.broadcasted_iota(jnp.int32, (n, HEAD_SIZE), 1)
        row = lax.broadcasted_iota(jnp.int32, (n, HEAD_SIZE), 0)
        angle = (row + place(s_id, first)).astype(F32) * freq[...]
        cos_t[lo:lo + n, :] = jnp.cos(angle)
        sn = jnp.sin(angle)
        sin_t[lo:lo + n, :] = jnp.where(lane < HEAD_SIZE // 2, -sn, sn)

    def kv_rows(zb, xb, lo, n):
        return kv.at[pl.ds((zb * X + xb) * R + lo, n), :]

    def col_copy(zb, p, target, sem):
        rows = kv_rows(zb, x, *pieces[p])
        return pltpu.make_async_remote_copy(
            src_ref=rows, dst_ref=rows, send_sem=sem, recv_sem=kc_sem.at[zb, p],
            device_id=(target, h_id), device_id_type=MESH,
        )

    def cross_copy(zb, xb, p, way, target, sem):
        rows = kv_rows(zb, xb, *pieces[p])
        return pltpu.make_async_remote_copy(
            src_ref=rows, dst_ref=rows, send_sem=sem, recv_sem=kx_sem.at[way - 1, zb, p],
            device_id=(target, h_id), device_id_type=MESH,
        )

    def send_x(zb, p):
        for k in range(1, X):
            cross_copy(zb, x, p, X - k, z * X + lax.rem(x + k, X), xs_sem).start()

    def send_up(zb, p):
        @pl.when(z < Z - 1)
        def _():
            col_copy(zb, p, s_id + X, zs_sem).start()

    def send_down(zb, p):
        @pl.when(z > 0)
        def _():
            col_copy(zb, p, s_id - X, zs_sem).start()

    def send_along(p, d):
        @pl.when(z + d < Z)
        def _():
            col_copy(z, p, s_id + d * X, zs_sem).start()

        @pl.when(z - d >= 0)
        def _():
            col_copy(z, p, s_id - d * X, zs_sem).start()

    def send_far(p):
        for d in range(2, Z):
            send_along(p, d)

    def send_own(p):
        send_along(p, 1)
        send_x(z, p)

    def pass_on(d, p):
        @pl.when(z - d >= 0)
        def _():
            col_copy(z - d, p, s_id, zs_sem).wait_recv()
            if p < 2:
                send_up(z - d, p)
            if d > 1 or p < 2:
                send_x(z - d, p)

        @pl.when(z + d < Z)
        def _():
            col_copy(z + d, p, s_id, zs_sem).wait_recv()
            if p < 2:
                send_down(z + d, p)
            if d > 1 or p < 2:
                send_x(z + d, p)

    def cross_wait(zb, way, p):
        cross_copy(zb, lax.rem(x + way, X), p, way, s_id, xs_sem).wait_recv()

    def cross_on(way, p):
        xb = lax.rem(x + way, X)
        cross_wait(z, way, p)

        @pl.when(z < Z - 1)
        def _():
            cross_copy(z, xb, p, way, s_id + X, zs_sem).start()

        @pl.when(z > 0)
        def _():
            cross_copy(z, xb, p, way, s_id - X, zs_sem).start()

    def store_kv(p):
        lo, n = pieces[p]
        got = jnp.dot(xg[lo:lo + n, :], wb[:, Cq:W], preferred_element_type=F32)
        turned = rotated(got[:, :Ck], cos_t[lo:lo + n, :], sin_t[lo:lo + n, :])
        rows = pl.ds(s_id * R + lo, n)
        for h in range(kv_heads):
            kv[rows, h * HEAD_SIZE:(h + 1) * HEAD_SIZE] = turned[h].astype(BF16)
        kv[rows, Ck:2 * Ck] = got[:, Ck:].astype(BF16)
        send_own(p)

    def store_q(u, side):
        lo, n = units[u]
        q = side[0]
        acc[0:n, :] = jnp.dot(xg[lo:lo + n, :], wb[:, :Cq], preferred_element_type=F32)
        turned = rotated(acc[0:n, :], cos_t[lo:lo + n, :], sin_t[lo:lo + n, :])
        for h in range(q_heads):
            at = (h % group) * n
            q[h // group, at:at + n, :] = turned[h].astype(BF16)

    wk_copy.wait()
    wv_copy.wait()
    store_kv(0)

    seg_copy.wait()
    starts = [
        jnp.sum(jnp.sum((seg[...] < v).astype(jnp.int32), axis=0, keepdims=True), axis=1, keepdims=True)
        for v in range(1, DOCS)
    ]
    for u, side in enumerate((near_side, far_side)):
        lo, n = units[u]
        info = side[5]
        for at, m, first in runs:
            if not lo <= at < lo + n:
                continue
            pos = lax.broadcasted_iota(jnp.int32, (1, m), 1) + place(s_id, first)
            start = jnp.zeros_like(pos)
            for begun in starts:
                start = jnp.where(begun <= pos, jnp.maximum(start, begun), start)
            for gh in range(info.shape[1] // n):
                lanes = slice(gh * n + at - lo, gh * n + at - lo + m)
                info[0:1, lanes] = pos
                info[1:2, lanes] = start
    for side in (far_side, near_side):
        side[1][...] = jnp.full_like(side[1], NEGATIVE_FILLER)
        side[2][...] = jnp.zeros_like(side[2])
        side[3][...] = jnp.zeros_like(side[3])

    hid_pair().wait_recv()
    store_kv(1)
    wo_copy.start()
    wq_copy.wait()
    store_q(0, near_side)

    scale = math.log2(math.e) / math.sqrt(HEAD_SIZE)
    nt = (((1,), (1,)), ((), ()))

    def attend(slot, u, side):
        q, m_s, l_s, o_s, bias, info = side
        chunk = bias.shape[1]
        lo, n = units[u]
        for at, m, first in runs:
            if not lo <= at < lo + n:
                continue
            kpos = lax.broadcasted_iota(jnp.int32, (m, chunk), 0) + place(slot, first)
            ok = (kpos <= info[0:1, :]) & (kpos >= info[1:2, :])
            bias[at - lo:at - lo + m, :] = jnp.where(ok, 0.0, NEGATIVE_FILLER)
        work = [(kh, w) for kh in range(kv_heads) for w in range(q.shape[1] // chunk)]
        span = lambda w: slice(w * chunk, (w + 1) * chunk)
        rows = pl.ds(slot * R + lo, n)
        keys = [kv[rows, kh * HEAD_SIZE:(kh + 1) * HEAD_SIZE] for kh in range(kv_heads)]
        vals = [
            kv[rows, Ck + kh * HEAD_SIZE:Ck + (kh + 1) * HEAD_SIZE].T for kh in range(kv_heads)
        ]

        def scores(item):
            kh, w = item
            return lax.dot_general(keys[kh], q[kh, span(w), :], nt, preferred_element_type=F32)

        ahead = scores(work[0])
        for i, (kh, w) in enumerate(work):
            raw = ahead
            if i + 1 < len(work):
                ahead = scores(work[i + 1])
            cols = span(w)
            s = raw * scale + bias[0:n, :]
            old = m_s[kh:kh + 1, cols]
            new = jnp.maximum(old, jnp.max(s, axis=0, keepdims=True))
            p = jnp.exp2(s - new)
            alpha = jnp.exp2(old - new)
            m_s[kh:kh + 1, cols] = new
            l_s[kh:kh + 1, cols] = l_s[kh:kh + 1, cols] * alpha + jnp.sum(p, axis=0, keepdims=True)
            o_s[kh, :, cols] = o_s[kh, :, cols] * alpha + jnp.dot(
                vals[kh], p.astype(BF16), preferred_element_type=F32
            )

    def visit(u, side, first, last, ways, wait):
        A, B = ways

        def one(i, _):
            d, rest_i = i // (2 * (B - A)), lax.rem(i, 2 * (B - A))
            sign, way = rest_i // (B - A), A + lax.rem(rest_i, B - A)
            zb = jnp.where(sign == 0, z - d, z + d)

            @pl.when((zb >= 0) & (zb < Z) & ((d > 0) | (sign == 0)))
            def _():
                if wait:
                    for p in wait:
                        cross_wait(zb, way, p)
                attend(zb * X + lax.rem(x + way, X), u, side)

            return 0

        lax.fori_loop(first * 2 * (B - A), last * 2 * (B - A), one, 0)

    def settle(side, lo):
        q, m_s, l_s, o_s, bias, info = side
        wide = q.shape[1] // group
        for h in range(q_heads):
            kh, gh = h // group, h % group
            lanes = slice(gh * wide, (gh + 1) * wide)
            att[lo:lo + wide, h * HEAD_SIZE:(h + 1) * HEAD_SIZE] = (
                o_s[kh, :, lanes] / l_s[kh:kh + 1, lanes]
            ).T.astype(BF16)

    column, others = (0, 1), (1, X)


    def relay(first, last, p):
        for d in range(first, min(last, Z)):
            pass_on(d, p)

    def hidden_on(e):
        for j in range(1, Y):
            hid_direct(j, e).wait_recv()
            hid_relay(j, e).start()

    def hidden_in(e):
        for j in range(1, Y):
            hid_relay(j, e).wait_recv()

    N_BOTH, F_BOTH = (0, 1), (2, 3)

    relay(1, 2, 0)
    visit(0, near_side, 0, 1, column, ())
    relay(1, 2, 1)
    visit(0, near_side, 1, min(2, Z), column, ())
    hidden_on(0)
    hidden_in(0)
    store_kv(2)
    relay(2, Z - 1, 0)
    relay(2, Z - 1, 1)
    send_far(2)
    visit(0, near_side, 0, 1, others, N_BOTH)
    visit(0, near_side, 2, Z - 1, column, ())
    visit(0, near_side, 1, min(2, Z), others, N_BOTH)
    hidden_on(1)
    hidden_in(1)
    store_kv(3)
    send_far(3)
    for way in range(1, X):
        cross_on(way, 2)
    store_q(1, far_side)
    visit(0, far_side, 0, min(2, Z), (0, X), ())
    relay(1, Z, 2)
    for way in range(1, X):
        cross_on(way, 3)
    visit(0, far_side, 2, Z - 1, column, ())
    visit(0, far_side, 2, Z - 1, others, N_BOTH)
    relay(1, Z, 3)
    relay(Z - 1, Z, 0)
    relay(Z - 1, Z, 1)
    visit(1, far_side, 0, 1, column, ())
    visit(1, far_side, 0, 1, others, ())
    visit(1, far_side, 1, Z, column, ())
    visit(0, far_side, Z - 1, Z, column, ())
    visit(0, far_side, Z - 1, Z, others, N_BOTH)
    visit(1, far_side, 1, Z, others, F_BOTH)
    settle(far_side, near_rows)
    wo_copy.wait()

    NW, PW = D // NO, D // NP

    def pair_far(j, n):
        cols = pl.ds(n * NW, NW)
        return pltpu.make_async_remote_copy(
            src_ref=give.at[j, :, cols], dst_ref=rb.at[j, :, cols],
            send_sem=ps_sem, recv_sem=pf_sem.at[j - 1, n],
            device_id=(s_id, partner), device_id_type=MESH,
        )

    def pair_near(n):
        cols = pl.ds(n * PW, PW)
        return pltpu.make_async_remote_copy(
            src_ref=give.at[0, :, cols], dst_ref=rb.at[0, :, cols],
            send_sem=ps_sem, recv_sem=pn_sem.at[n],
            device_id=(s_id, partner), device_id_type=MESH,
        )

    def far_copy(j, n):
        cols = pl.ds(n * NW, NW)
        return pltpu.make_async_remote_copy(
            src_ref=sb.at[j - 1, :, cols], dst_ref=fb.at[j - 1, :, cols],
            send_sem=ys_sem, recv_sem=yr_sem.at[j - 1, n],
            device_id=(s_id, peer_y(j) * CORES + c), device_id_type=MESH,
        )

    def project_far(n, _):
        @pl.when(n < NO)
        def _():
            cols = pl.ds(n * NW, NW)
            got = jnp.dot(att[near_rows:R, :], wo[:, cols], preferred_element_type=F32).astype(BF16)
            for j in range(1, Y):
                for e in range(2):
                    at = far_at(j, e) - near_rows
                    keep[j, e * part:(e + 1) * part, cols] = got[at:at + part, :]
                    give[j, e * part:(e + 1) * part, cols] = got[at + part:at + r, :]
                pair_far(j, n).start()

        @pl.when(n >= LAG)
        def _():
            cols = pl.ds((n - LAG) * NW, NW)
            for j in range(1, Y):
                pair_far(j, n - LAG).wait_recv()
                sb[j - 1, :, cols] = (keep[j, :, cols].astype(F32) + rb[j, :, cols].astype(F32)).astype(BF16)
                far_copy(j, n - LAG).start()

        return 0

    lax.fori_loop(0, NO + LAG, project_far, 0)
    visit(0, near_side, 3, Z, column, ())
    visit(0, near_side, 2, Z, others, ())
    visit(1, near_side, 0, Z, (0, X), ())
    settle(near_side, 0)

    def project_near(n, _):
        cols = pl.ds(n * PW, PW)
        got = jnp.dot(att[0:near_rows, :], wo[:, cols], preferred_element_type=F32).astype(BF16)
        keep[0, :, cols] = got[:r, :]
        give[0, :, cols] = got[r:, :]
        pair_near(n).start()
        return 0

    lax.fori_loop(0, NP, project_near, 0)

    for n in range(NP):
        pair_near(n).wait_recv()

    def finish(n, _):
        cols = pl.ds(n * NW, NW)
        total = keep[0, :, cols].astype(F32) + rb[0, :, cols].astype(F32)
        for j in range(1, Y):
            far_copy(j, n).wait_recv()
            total = total + fb[j - 1, :, cols].astype(F32)
        out[:, cols] = total.astype(BF16)
        return 0

    lax.fori_loop(0, NO, finish, 0)

    def drain(ref, sem):
        pltpu.make_async_copy(ref, ref, sem).wait()

    drain(xg.at[pl.ds(0, (2 * Y - 1) * r), :], hs_sem)
    drain(give, ps_sem)
    drain(sb, ys_sem)
    for zz in range(Z):
        ups, downs = (zz + 1 if zz < Z - 1 else 0), (Z - zz if zz > 0 else 0)
        beside = (zz > 0) + (zz < Z - 1)
        along = (ups + downs) * near_rows + (Z - 1 + (X - 1) * beside) * far_rows
        over = (X - 1) * (Z * R - beside * far_rows)

        @pl.when(z == zz)
        def _(along=along, over=over):
            drain(kv.at[pl.ds(0, along), :], zs_sem)
            drain(kv.at[pl.ds(0, over), :], xs_sem)


def on_device(X, Z, Y, hidden, block_order, segment_ids, w_query, key_weight, value_weight, w_out):
    r, D = hidden.shape
    S, H = X * Z, Y * CORES
    R = r * H
    Cq, Ck = w_query.shape[1], key_weight.shape[1]
    W = Cq + 2 * Ck
    q_heads = Cq // HEAD_SIZE
    NO, NP = max(1, D // 512), max(1, D // 1024)
    exponent = np.arange(HEAD_SIZE // 2, dtype=np.float64) * 2.0 / HEAD_SIZE
    freqs = np.tile(ROPE_BASE ** (-exponent), 2).astype(np.float32)[None, :]
    dma = pltpu.SemaphoreType.DMA
    kv_heads = Ck // HEAD_SIZE
    group = q_heads // kv_heads
    near_rows, far_rows = CORES * r, R - CORES * r
    segments = segment_ids.reshape(block_order.shape[0], -1)

    def half_scratch(rows):
        together = 2 if rows % HEAD_SIZE == 0 and group % 2 == 0 else group
        lanes = group * rows
        return [
            pltpu.VMEM((kv_heads, lanes, HEAD_SIZE), BF16),
            pltpu.VMEM((kv_heads, lanes), F32),
            pltpu.VMEM((kv_heads, lanes), F32),
            pltpu.VMEM((kv_heads, HEAD_SIZE, lanes), F32),
            pltpu.VMEM((max(near_rows, far_rows), together * rows), F32),
            pltpu.VMEM((2, together * rows), jnp.int32),
        ]

    far = max(1, Y - 1)
    anywhere = pl.BlockSpec(memory_space=pl.ANY)
    return pl.pallas_call(
        functools.partial(kernel, X, Z, Y, NO, NP),
        out_shape=pltpu.VMEM((r, D), BF16),
        in_specs=[pl.BlockSpec(memory_space=pltpu.SMEM)] + [anywhere] * 7,
        out_specs=pl.BlockSpec(memory_space=pltpu.VMEM),
        scratch_shapes=[
            pltpu.VMEM(segments.shape, jnp.int32),
            pltpu.VMEM((1, HEAD_SIZE), F32),
            pltpu.VMEM((R, D), BF16),
            pltpu.VMEM((D, W), BF16),
            pltpu.VMEM((Cq, D), BF16),
            pltpu.VMEM((max(near_rows, far_rows), Cq), F32),
            pltpu.VMEM((R, HEAD_SIZE), F32),
            pltpu.VMEM((R, HEAD_SIZE), F32),
            pltpu.VMEM((S * R, 2 * Ck), BF16),
            pltpu.VMEM((R, Cq), BF16),
            pltpu.VMEM((Y, r, D), BF16),
            pltpu.VMEM((Y, r, D), BF16),
            pltpu.VMEM((Y, r, D), BF16),
            pltpu.VMEM((far, r, D), BF16),
            pltpu.VMEM((far, r, D), BF16),
            *half_scratch(far_rows),
            *half_scratch(near_rows),
            dma((2,)), dma, dma((2,)), dma, dma,
            dma, dma, dma((far, 2)), dma((far, 2)),
            dma, dma, dma((Z, 4)), dma((max(1, X - 1), Z, 4)),
            dma, dma((far, NO)), dma((NP,)), dma, dma((far, NO)),
        ],
        compiler_params=pltpu.CompilerParams(
            collective_id=0, has_side_effects=True, vmem_limit_bytes=60 * 1024 * 1024
        ),
    )(
        block_order, hidden, segments, jnp.asarray(freqs),
        w_query, key_weight, value_weight, w_out,
    )


def solution(mesh):
    seq, head = mesh.shape["seq"], mesh.shape["head"]
    X = 1
    while 4 * X * X <= seq and seq % (2 * X) == 0:
        X *= 2
    placed = (
        P(("seq", "head"), None),
        P(),
        P(),
        P(None, "head"),
        P(None, "head"),
        P(None, "head"),
        P("head", None),
    )
    return jax.shard_map(
        functools.partial(on_device, X, seq // X, head // CORES),
        mesh=mesh, in_specs=placed, out_specs=P(("seq", "head"), None), check_vma=False,
    )
```

```python
import functools
import math

import jax
import jax.numpy as jnp
import numpy as np
from jax import lax
from jax.experimental import pallas as pl
from jax.experimental.pallas import tpu as pltpu
from jax.sharding import PartitionSpec as P

HEAD_SIZE = 128
NEGATIVE_FILLER = -1e30
ROPE_BASE = 500000.0
DOCS = 4
CORES = 2
LAG = 3
AHEAD = 2
MESH = pl.DeviceIdType.MESH
F32 = jnp.float32
BF16 = jnp.bfloat16


def rotated(t, cosine, sine):
    heads = t.shape[1] // HEAD_SIZE
    pieces = []
    for h in range(heads):
        one = t[:, h * HEAD_SIZE:(h + 1) * HEAD_SIZE]
        pieces.append(one * cosine + pltpu.roll(one, HEAD_SIZE // 2, 1) * sine)
    return pieces


def kernel(
    X, Z, Y, PARTS, NO, NP,
    order, hidden, seg_hbm, freq_hbm, wq, wk, wv, wo_hbm, out,
    seg, freq, xg, wb, wo, acc, cos_t, sin_t, kv, att, keep, give, rb, sb, fb, *rest,
):
    far_side, near_side = rest[:6], rest[6:12]
    (in_sem, hn_sem, wkv_sem, wq_sem, wo_sem, hs_sem, hp_sem, hd_sem, hr_sem,
     xs_sem, zs_sem, kc_sem, kx_sem, ps_sem, pf_sem, pn_sem, ys_sem, yr_sem, ready) = rest[12:]
    r, D = hidden.shape
    R = xg.shape[0]
    Cq, Ck = wq.shape[1], wk.shape[1]
    half = R // 2
    q_heads, kv_heads = Cq // HEAD_SIZE, Ck // HEAD_SIZE
    group = q_heads // kv_heads
    W = Cq + 2 * Ck
    near_rows, far_rows = CORES * r, R - CORES * r
    part = r // PARTS
    wide_part = (Y - 1) * CORES * part
    S = X * Z
    TOGETHER = math.gcd(S, 4)
    s_id, h_id = lax.axis_index("seq"), lax.axis_index("head")
    y, c = h_id // CORES, h_id % CORES
    z, x = s_id // X, s_id % X
    partner = y * CORES + (1 - c)

    def peer_y(j):
        return lax.rem(y + j, Y)

    def far_at(j, e):
        return near_rows + e * wide_part + (j - 1) * CORES * part

    runs = [(0, r, h_id * r), (r, r, partner * r)]
    for e in range(PARTS):
        for j in range(1, Y):
            for i, core in enumerate((c, 1 - c)):
                runs.append((far_at(j, e) + i * part, part, (peer_y(j) * CORES + core) * r + e * part))
    pieces = [(0, r), (r, r)] + [(near_rows + e * wide_part, wide_part) for e in range(PARTS)]
    units = [(0, near_rows), (near_rows, far_rows)]

    def place(slot, first):
        return order[2 * slot + first // half] * half + lax.rem(first, half)

    barrier = pltpu.get_barrier_semaphore()

    def greet(sq, hd):
        pl.semaphore_signal(barrier, inc=1, device_id=(sq, hd), device_id_type=MESH)

    greet(s_id, partner)
    for j in range(1, Y):
        greet(s_id, peer_y(j) * CORES + c)
    for k in range(1, X):
        greet(z * X + lax.rem(x + k, X), h_id)

    @pl.when(z > 0)
    def _():
        greet(s_id - X, h_id)

    @pl.when(z < Z - 1)
    def _():
        greet(s_id + X, h_id)

    own_rows = pltpu.make_async_copy(hidden, xg.at[pl.ds(0, r), :], hn_sem)
    own_rows.start()
    seg_copy = pltpu.make_async_copy(seg_hbm, seg, in_sem.at[0])
    freq_copy = pltpu.make_async_copy(freq_hbm, freq, in_sem.at[1])
    freq_copy.start()
    seg_copy.start()
    wk_copy = pltpu.make_async_copy(wk, wb.at[:, pl.ds(Cq, Ck)], wkv_sem.at[0])
    wv_copy = pltpu.make_async_copy(wv, wb.at[:, pl.ds(Cq + Ck, Ck)], wkv_sem.at[1])
    wq_copy = pltpu.make_async_copy(wq, wb.at[:, pl.ds(0, Cq)], wq_sem)
    wo_copy = pltpu.make_async_copy(wo_hbm, wo, wo_sem)
    wk_copy.start()
    wv_copy.start()

    near = jnp.where(z > 0, 1, 0) + jnp.where(z < Z - 1, 1, 0)
    pl.semaphore_wait(barrier, 1 + (Y - 1) + (X - 1) + near)

    def tell(side, ok):
        @pl.when(ok)
        def _():
            pl.semaphore_signal(
                ready.at[side], inc=1, device_id=(s_id + (X if side == 0 else -X), h_id),
                device_id_type=MESH,
            )

    def hear(d):
        for side, there in ((0, z - d >= 0), (1, z + d < Z)):
            @pl.when(there)
            def _(side=side):
                pl.semaphore_wait(ready.at[side], 1)

            tell(side, there & ((z < Z - 1) if side == 0 else (z > 0)))

    tell(0, (z > 0) & (z < Z - 1))
    tell(1, (z < Z - 1) & (z > 0))

    def hid_pair():
        return pltpu.make_async_remote_copy(
            src_ref=xg.at[pl.ds(0, r), :], dst_ref=xg.at[pl.ds(r, r), :],
            send_sem=hs_sem, recv_sem=hp_sem,
            device_id=(s_id, partner), device_id_type=MESH,
        )

    def hid_send(j, e):
        return pltpu.make_async_remote_copy(
            src_ref=xg.at[pl.ds(e * part, part), :], dst_ref=xg.at[pl.ds(far_at(Y - j, e), part), :],
            send_sem=hs_sem, recv_sem=hd_sem.at[Y - j - 1, e],
            device_id=(s_id, peer_y(j) * CORES + c), device_id_type=MESH,
        )

    def hid_direct(j, e):
        rows = xg.at[pl.ds(far_at(j, e), part), :]
        return pltpu.make_async_remote_copy(
            src_ref=rows, dst_ref=rows, send_sem=hs_sem, recv_sem=hd_sem.at[j - 1, e],
            device_id=(s_id, partner), device_id_type=MESH,
        )

    def hid_relay(j, e):
        return pltpu.make_async_remote_copy(
            src_ref=xg.at[pl.ds(far_at(j, e), part), :],
            dst_ref=xg.at[pl.ds(far_at(j, e) + part, part), :],
            send_sem=hs_sem, recv_sem=hr_sem.at[j - 1, e],
            device_id=(s_id, partner), device_id_type=MESH,
        )

    own_rows.wait()
    hid_pair().start()
    for e in range(PARTS):
        for j in range(1, Y):
            hid_send(j, e).start()
    wq_copy.start()

    freq_copy.wait()
    for lo, n, first in runs:
        lane = lax.broadcasted_iota(jnp.int32, (n, HEAD_SIZE), 1)
        row = lax.broadcasted_iota(jnp.int32, (n, HEAD_SIZE), 0)
        angle = (row + place(s_id, first)).astype(F32) * freq[...]
        cos_t[lo:lo + n, :] = jnp.cos(angle)
        sn = jnp.sin(angle)
        sin_t[lo:lo + n, :] = jnp.where(lane < HEAD_SIZE // 2, -sn, sn)

    def kv_rows(zb, xb, lo, n):
        return kv.at[pl.ds((zb * X + xb) * R + lo, n), :]

    def col_copy(zb, p, target, sem):
        rows = kv_rows(zb, x, *pieces[p])
        return pltpu.make_async_remote_copy(
            src_ref=rows, dst_ref=rows, send_sem=sem, recv_sem=kc_sem.at[zb, p],
            device_id=(target, h_id), device_id_type=MESH,
        )

    def cross_copy(zb, xb, p, way, target, sem):
        rows = kv_rows(zb, xb, *pieces[p])
        return pltpu.make_async_remote_copy(
            src_ref=rows, dst_ref=rows, send_sem=sem, recv_sem=kx_sem.at[way - 1, zb, p],
            device_id=(target, h_id), device_id_type=MESH,
        )

    def send_x(zb, p):
        for k in range(1, X):
            cross_copy(zb, x, p, X - k, z * X + lax.rem(x + k, X), xs_sem).start()

    def send_up(zb, p):
        @pl.when(z < Z - 1)
        def _():
            col_copy(zb, p, s_id + X, zs_sem).start()

    def send_down(zb, p):
        @pl.when(z > 0)
        def _():
            col_copy(zb, p, s_id - X, zs_sem).start()

    def send_along(p, d):
        @pl.when(z + d < Z)
        def _():
            col_copy(z, p, s_id + d * X, zs_sem).start()

        @pl.when(z - d >= 0)
        def _():
            col_copy(z, p, s_id - d * X, zs_sem).start()

    def send_own(p):
        for d in range(1 if p < 2 else Z - 1, 0, -1):
            send_along(p, d)
        send_x(z, p)

    def at_end(a, b):
        return (a == 0) | (a == Z - 1) | (b == 0) | (b == Z - 1)

    def pass_on(d, p):
        for side, zb, there in ((0, z - d, z - d >= 0), (1, z + d, z + d < Z)):
            @pl.when(there)
            def _(side=side, zb=zb):
                col_copy(zb, p, s_id, zs_sem).wait_recv()
                if p < 2 and d == 1:
                    (send_up if side == 0 else send_down)(zb, p)
                if p < 2 or d > 1:
                    send_x(zb, p)
                else:
                    @pl.when(jnp.logical_not(at_end(z, zb)))
                    def _():
                        send_x(zb, p)

    def cross_wait(zb, way, p):
        cross_copy(zb, lax.rem(x + way, X), p, way, s_id, xs_sem).wait_recv()

    def cross_on(way, p):
        xb = lax.rem(x + way, X)
        cross_wait(z, way, p)

        @pl.when((z < Z - 1) & at_end(z, z + 1))
        def _():
            cross_copy(z, xb, p, way, s_id + X, zs_sem).start()

        @pl.when((z > 0) & at_end(z, z - 1))
        def _():
            cross_copy(z, xb, p, way, s_id - X, zs_sem).start()

    def store_kv(p):
        lo, n = pieces[p]
        got = jnp.dot(xg[lo:lo + n, :], wb[:, Cq:W], preferred_element_type=F32)
        turned = rotated(got[:, :Ck], cos_t[lo:lo + n, :], sin_t[lo:lo + n, :])
        rows = pl.ds(s_id * R + lo, n)
        for h in range(kv_heads):
            kv[rows, h * HEAD_SIZE:(h + 1) * HEAD_SIZE] = turned[h].astype(BF16)
        kv[rows, Ck:2 * Ck] = got[:, Ck:].astype(BF16)
        send_own(p)

    def store_q(u, side):
        lo, n = units[u]
        q = side[0]
        acc[0:n, :] = jnp.dot(xg[lo:lo + n, :], wb[:, :Cq], preferred_element_type=F32)
        turned = rotated(acc[0:n, :], cos_t[lo:lo + n, :], sin_t[lo:lo + n, :])
        for h in range(q_heads):
            at = (h % group) * n
            q[h // group, at:at + n, :] = turned[h].astype(BF16)

    wk_copy.wait()
    wv_copy.wait()
    store_kv(0)

    seg_copy.wait()
    starts = [
        jnp.sum(jnp.sum((seg[...] < v).astype(jnp.int32), axis=0, keepdims=True), axis=1, keepdims=True)
        for v in range(1, DOCS)
    ]
    for u, side in enumerate((near_side, far_side)):
        lo, n = units[u]
        info = side[5]
        for at, m, first in runs:
            if not lo <= at < lo + n:
                continue
            pos = lax.broadcasted_iota(jnp.int32, (1, m), 1) + place(s_id, first)
            start = jnp.zeros_like(pos)
            for begun in starts:
                start = jnp.where(begun <= pos, jnp.maximum(start, begun), start)
            for gh in range(info.shape[1] // n):
                lanes = slice(gh * n + at - lo, gh * n + at - lo + m)
                info[0:1, lanes] = pos
                info[1:2, lanes] = start
    for side in (far_side, near_side):
        side[1][...] = jnp.full_like(side[1], NEGATIVE_FILLER)
        side[2][...] = jnp.zeros_like(side[2])
        side[3][...] = jnp.zeros_like(side[3])

    hid_pair().wait_recv()
    store_kv(1)
    for d in range(2, min(3, Z)):
        hear(d)
    wo_copy.start()
    wq_copy.wait()
    store_q(0, near_side)

    scale = math.log2(math.e) / math.sqrt(HEAD_SIZE)
    nt = (((1,), (1,)), ((), ()))

    def nearest(n):
        low = jnp.minimum(z, Z - 1 - z)
        d = (n + 1) // 2
        both = jnp.where(lax.rem(n, 2) == 1, z - d, z + d)
        return jnp.where(n <= 2 * low, both, jnp.where(z < Z - 1 - z, n, Z - 1 - n))

    def attend(slots, u, side):
        q, m_s, l_s, o_s, bias, info = side
        chunk = bias.shape[1]
        lo, n = units[u]
        total = len(slots) * n
        for t, slot in enumerate(slots):
            for at, m, first in runs:
                if not lo <= at < lo + n:
                    continue
                kpos = lax.broadcasted_iota(jnp.int32, (m, chunk), 0) + place(slot, first)
                ok = (kpos <= info[0:1, :]) & (kpos >= info[1:2, :])
                bias[t * n + at - lo:t * n + at - lo + m, :] = jnp.where(ok, 0.0, NEGATIVE_FILLER)
        work = [(kh, w) for kh in range(kv_heads) for w in range(q.shape[1] // chunk)]
        span = lambda w: slice(w * chunk, (w + 1) * chunk)

        def gathered(col):
            cols = slice(col, col + HEAD_SIZE)
            return jnp.concatenate([kv[pl.ds(slot * R + lo, n), cols] for slot in slots], axis=0)

        keys = [gathered(kh * HEAD_SIZE) for kh in range(kv_heads)]
        vals = [gathered(Ck + kh * HEAD_SIZE).T for kh in range(kv_heads)]

        def scores(item):
            kh, w = item
            return lax.dot_general(keys[kh], q[kh, span(w), :], nt, preferred_element_type=F32)

        ahead = [scores(item) for item in work[:AHEAD]]
        for i, (kh, w) in enumerate(work):
            raw = ahead.pop(0)
            if i + AHEAD < len(work):
                ahead.append(scores(work[i + AHEAD]))
            cols = span(w)
            s = raw * scale + bias[0:total, :]
            old = m_s[kh:kh + 1, cols]
            new = jnp.maximum(old, jnp.max(s, axis=0, keepdims=True))
            p = jnp.exp2(s - new)
            alpha = jnp.exp2(old - new)
            m_s[kh:kh + 1, cols] = new
            l_s[kh:kh + 1, cols] = l_s[kh:kh + 1, cols] * alpha + jnp.sum(p, axis=0, keepdims=True)
            o_s[kh, :, cols] = o_s[kh, :, cols] * alpha + jnp.dot(
                vals[kh], p.astype(BF16), preferred_element_type=F32
            )

    def visit(u, side, first, last):
        def one(i, _):
            slots = []
            for t in range(TOGETHER):
                i_t = i * TOGETHER + t
                slots.append(nearest(i_t // X) * X + lax.rem(x + lax.rem(i_t, X), X))
            attend(slots, u, side)
            return 0

        lax.fori_loop(first // TOGETHER, last // TOGETHER, one, 0)

    def settle(side, lo):
        q, m_s, l_s, o_s, bias, info = side
        wide = q.shape[1] // group
        for h in range(q_heads):
            kh, gh = h // group, h % group
            lanes = slice(gh * wide, (gh + 1) * wide)
            att[lo:lo + wide, h * HEAD_SIZE:(h + 1) * HEAD_SIZE] = (
                o_s[kh, :, lanes] / l_s[kh:kh + 1, lanes]
            ).T.astype(BF16)

    column, others = (0, 1), (1, X)


    def relay(first, last, p):
        for d in range(first, min(last, Z)):
            pass_on(d, p)

    def hidden_on(e):
        for j in range(1, Y):
            hid_direct(j, e).wait_recv()
            hid_relay(j, e).start()

    def hidden_in(e):
        for j in range(1, Y):
            hid_relay(j, e).wait_recv()

    def crossed(first, last, parts):
        for n in range(first, last):
            for way in range(1, X):
                for p in parts:
                    cross_wait(nearest(jnp.int32(n)), way, p)

    N_ALL, F_ALL = (0, 1), tuple(range(2, 2 + PARTS))
    last = PARTS - 1

    for d in range(3, Z):
        hear(d)
        send_along(0, d)
        send_along(1, d)
    relay(1, 2, 0)
    relay(1, 2, 1)
    for e in range(PARTS):
        if e == last:
            relay(2, 3, 0)
            relay(3, Z, 0)
            relay(3, Z, 1)
            relay(2, 3, 1)
        hidden_on(e)
        hidden_in(e)
        store_kv(2 + e)
    for p in F_ALL[:-1]:
        for way in range(1, X):
            cross_on(way, p)
    store_q(1, far_side)
    crossed(0, 2, N_ALL)
    visit(0, far_side, 0, S // 2)
    for p in F_ALL[:-1]:
        for d in range(Z - 1, 0, -1):
            relay(d, d + 1, p)
    for way in range(1, X):
        cross_on(way, 1 + PARTS)
    for d in range(Z - 1, 0, -1):
        relay(d, d + 1, 1 + PARTS)
    crossed(2, Z, N_ALL)
    visit(0, far_side, S // 2, S)
    crossed(1, 2, F_ALL)
    visit(1, far_side, 0, S // 2)
    crossed(2, Z, F_ALL)
    visit(1, far_side, S // 2, S)
    settle(far_side, near_rows)
    wo_copy.wait()

    NW, PW = D // NO, D // NP

    def pair_far(j, n):
        cols = pl.ds(n * NW, NW)
        return pltpu.make_async_remote_copy(
            src_ref=give.at[j, :, cols], dst_ref=rb.at[j, :, cols],
            send_sem=ps_sem, recv_sem=pf_sem.at[j - 1, n],
            device_id=(s_id, partner), device_id_type=MESH,
        )

    def pair_near(n):
        cols = pl.ds(n * PW, PW)
        return pltpu.make_async_remote_copy(
            src_ref=give.at[0, :, cols], dst_ref=rb.at[0, :, cols],
            send_sem=ps_sem, recv_sem=pn_sem.at[n],
            device_id=(s_id, partner), device_id_type=MESH,
        )

    def far_copy(j, n):
        cols = pl.ds(n * NW, NW)
        return pltpu.make_async_remote_copy(
            src_ref=sb.at[j - 1, :, cols], dst_ref=fb.at[j - 1, :, cols],
            send_sem=ys_sem, recv_sem=yr_sem.at[j - 1, n],
            device_id=(s_id, peer_y(j) * CORES + c), device_id_type=MESH,
        )

    def project_far(n, _):
        @pl.when(n < NO)
        def _():
            cols = pl.ds(n * NW, NW)
            got = jnp.dot(att[near_rows:R, :], wo[:, cols], preferred_element_type=F32).astype(BF16)
            for j in range(1, Y):
                for e in range(PARTS):
                    at = far_at(j, e) - near_rows
                    keep[j, e * part:(e + 1) * part, cols] = got[at:at + part, :]
                    give[j, e * part:(e + 1) * part, cols] = got[at + part:at + 2 * part, :]
                pair_far(j, n).start()

        @pl.when(n >= LAG)
        def _():
            cols = pl.ds((n - LAG) * NW, NW)
            for j in range(1, Y):
                pair_far(j, n - LAG).wait_recv()
                sb[j - 1, :, cols] = (keep[j, :, cols].astype(F32) + rb[j, :, cols].astype(F32)).astype(BF16)
                far_copy(j, n - LAG).start()

        return 0

    lax.fori_loop(0, NO + LAG, project_far, 0)
    visit(0, near_side, 0, S)
    visit(1, near_side, 0, S)
    settle(near_side, 0)

    def project_near(n, _):
        cols = pl.ds(n * PW, PW)
        got = jnp.dot(att[0:near_rows, :], wo[:, cols], preferred_element_type=F32).astype(BF16)
        keep[0, :, cols] = got[:r, :]
        give[0, :, cols] = got[r:, :]
        pair_near(n).start()
        return 0

    lax.fori_loop(0, NP, project_near, 0)

    for n in range(NP):
        pair_near(n).wait_recv()

    def finish(n, _):
        cols = pl.ds(n * NW, NW)
        total = keep[0, :, cols].astype(F32) + rb[0, :, cols].astype(F32)
        for j in range(1, Y):
            far_copy(j, n).wait_recv()
            total = total + fb[j - 1, :, cols].astype(F32)
        out[:, cols] = total.astype(BF16)
        return 0

    lax.fori_loop(0, NO, finish, 0)

    def drain(ref, sem):
        pltpu.make_async_copy(ref, ref, sem).wait()

    drain(xg.at[pl.ds(0, (2 * Y - 1) * r), :], hs_sem)
    drain(give, ps_sem)
    drain(sb, ys_sem)
    for zz in range(Z):
        ends = (0, Z - 1)
        beside = [zb for zb in (zz - 1, zz + 1) if 0 <= zb < Z]
        bent = sum(zz in ends or zb in ends for zb in beside)
        early = len(beside) + 2 * (len(beside) == 2) + max(0, zz - 2) + max(0, Z - 3 - zz)
        along = early * near_rows + (Z - 1 + (X - 1) * bent) * far_rows
        over = (X - 1) * (Z * R - bent * far_rows)

        @pl.when(z == zz)
        def _(along=along, over=over):
            drain(kv.at[pl.ds(0, along), :], zs_sem)
            drain(kv.at[pl.ds(0, over), :], xs_sem)


def on_device(X, Z, Y, hidden, block_order, segment_ids, w_query, key_weight, value_weight, w_out):
    r, D = hidden.shape
    S, H = X * Z, Y * CORES
    R = r * H
    Cq, Ck = w_query.shape[1], key_weight.shape[1]
    W = Cq + 2 * Ck
    q_heads = Cq // HEAD_SIZE
    NO, NP = max(1, D // 512), max(1, D // 1024)
    PARTS = max(1, min(2, r // 16))
    exponent = np.arange(HEAD_SIZE // 2, dtype=np.float64) * 2.0 / HEAD_SIZE
    freqs = np.tile(ROPE_BASE ** (-exponent), 2).astype(np.float32)[None, :]
    dma = pltpu.SemaphoreType.DMA
    kv_heads = Ck // HEAD_SIZE
    group = q_heads // kv_heads
    near_rows, far_rows = CORES * r, R - CORES * r
    segments = segment_ids.reshape(block_order.shape[0], -1)

    def half_scratch(rows):
        together = 1 if rows % HEAD_SIZE == 0 else group
        lanes = group * rows
        return [
            pltpu.VMEM((kv_heads, lanes, HEAD_SIZE), BF16),
            pltpu.VMEM((kv_heads, lanes), F32),
            pltpu.VMEM((kv_heads, lanes), F32),
            pltpu.VMEM((kv_heads, HEAD_SIZE, lanes), F32),
            pltpu.VMEM((math.gcd(S, 4) * max(near_rows, far_rows), together * rows), F32),
            pltpu.VMEM((2, together * rows), jnp.int32),
        ]

    far = max(1, Y - 1)
    anywhere = pl.BlockSpec(memory_space=pl.ANY)
    return pl.pallas_call(
        functools.partial(kernel, X, Z, Y, PARTS, NO, NP),
        out_shape=pltpu.VMEM((r, D), BF16),
        in_specs=[pl.BlockSpec(memory_space=pltpu.SMEM)] + [anywhere] * 7,
        out_specs=pl.BlockSpec(memory_space=pltpu.VMEM),
        scratch_shapes=[
            pltpu.VMEM(segments.shape, jnp.int32),
            pltpu.VMEM((1, HEAD_SIZE), F32),
            pltpu.VMEM((R, D), BF16),
            pltpu.VMEM((D, W), BF16),
            pltpu.VMEM((Cq, D), BF16),
            pltpu.VMEM((max(near_rows, far_rows), Cq), F32),
            pltpu.VMEM((R, HEAD_SIZE), F32),
            pltpu.VMEM((R, HEAD_SIZE), F32),
            pltpu.VMEM((S * R, 2 * Ck), BF16),
            pltpu.VMEM((R, Cq), BF16),
            pltpu.VMEM((Y, r, D), BF16),
            pltpu.VMEM((Y, r, D), BF16),
            pltpu.VMEM((Y, r, D), BF16),
            pltpu.VMEM((far, r, D), BF16),
            pltpu.VMEM((far, r, D), BF16),
            *half_scratch(far_rows),
            *half_scratch(near_rows),
            dma((2,)), dma, dma((2,)), dma, dma,
            dma, dma, dma((far, PARTS)), dma((far, PARTS)),
            dma, dma, dma((Z, 2 + PARTS)), dma((max(1, X - 1), Z, 2 + PARTS)),
            dma, dma((far, NO)), dma((NP,)), dma, dma((far, NO)),
            pltpu.SemaphoreType.REGULAR((2,)),
        ],
        compiler_params=pltpu.CompilerParams(
            collective_id=0, has_side_effects=True, vmem_limit_bytes=60 * 1024 * 1024
        ),
    )(
        block_order, hidden, segments, jnp.asarray(freqs),
        w_query, key_weight, value_weight, w_out,
    )


def solution(mesh):
    seq, head = mesh.shape["seq"], mesh.shape["head"]
    X = 1
    while 4 * X * X <= seq and seq % (2 * X) == 0:
        X *= 2
    placed = (
        P(("seq", "head"), None),
        P(),
        P(),
        P(None, "head"),
        P(None, "head"),
        P(None, "head"),
        P("head", None),
    )
    return jax.shard_map(
        functools.partial(on_device, X, seq // X, head // CORES),
        mesh=mesh, in_specs=placed, out_specs=P(("seq", "head"), None), check_vma=False,
    )
```

```python
import functools
import math

import jax
import jax.numpy as jnp
import numpy as np
from jax import lax
from jax.experimental import pallas as pl
from jax.experimental.pallas import tpu as pltpu
from jax.sharding import PartitionSpec as P

HEAD_SIZE = 128
NEGATIVE_FILLER = -1e30
ROPE_BASE = 500000.0
DOCS = 4
CORES = 2
LAG = 3
AHEAD = 2
MESH = pl.DeviceIdType.MESH
F32 = jnp.float32
BF16 = jnp.bfloat16


def rotated(t, cosine, sine):
    heads = t.shape[1] // HEAD_SIZE
    pieces = []
    for h in range(heads):
        one = t[:, h * HEAD_SIZE:(h + 1) * HEAD_SIZE]
        pieces.append(one * cosine + pltpu.roll(one, HEAD_SIZE // 2, 1) * sine)
    return pieces


def kernel(
    X, Z, Y, PARTS, NO, NP,
    order_hbm, hidden, seg_hbm, freq_hbm, wq, wk, wv, wo_hbm, out,
    order, seg, freq, xg, wb, wo, acc, cos_t, sin_t, kv, att, keep, give, rb, sb, fb, *rest,
):
    far_side, near_side = rest[:6], rest[6:12]
    (in_sem, hn_sem, wkv_sem, wq_sem, wo_sem, hs_sem, hp_sem, hd_sem, hr_sem,
     xs_sem, zs_sem, kc_sem, kx_sem, ps_sem, pf_sem, pn_sem, ys_sem, yr_sem, ready) = rest[12:]
    r, D = hidden.shape
    R = xg.shape[0]
    Cq, Ck = wq.shape[1], wk.shape[1]
    half = R // 2
    q_heads, kv_heads = Cq // HEAD_SIZE, Ck // HEAD_SIZE
    group = q_heads // kv_heads
    W = Cq + 2 * Ck
    near_rows, far_rows = CORES * r, R - CORES * r
    part = r // PARTS
    wide_part = (Y - 1) * CORES * part
    S = X * Z
    TOGETHER = math.gcd(S, 4)
    s_id, h_id = lax.axis_index("seq"), lax.axis_index("head")
    y, c = h_id // CORES, h_id % CORES
    z, x = s_id // X, s_id % X
    partner = y * CORES + (1 - c)

    def peer_y(j):
        return lax.rem(y + j, Y)

    def far_at(j, e):
        return near_rows + e * wide_part + (j - 1) * CORES * part

    runs = [(0, r, h_id * r), (r, r, partner * r)]
    for e in range(PARTS):
        for j in range(1, Y):
            for i, core in enumerate((c, 1 - c)):
                runs.append((far_at(j, e) + i * part, part, (peer_y(j) * CORES + core) * r + e * part))
    pieces = [(0, r), (r, r)] + [(near_rows + e * wide_part, wide_part) for e in range(PARTS)]
    units = [(0, near_rows), (near_rows, far_rows)]

    def place(slot, first):
        return order[2 * slot + first // half] * half + lax.rem(first, half)

    barrier = pltpu.get_barrier_semaphore()

    def greet(sq, hd):
        pl.semaphore_signal(barrier, inc=1, device_id=(sq, hd), device_id_type=MESH)

    greet(s_id, partner)
    for j in range(1, Y):
        greet(s_id, peer_y(j) * CORES + c)
    for k in range(1, X):
        greet(z * X + lax.rem(x + k, X), h_id)

    @pl.when(z > 0)
    def _():
        greet(s_id - X, h_id)

    @pl.when(z < Z - 1)
    def _():
        greet(s_id + X, h_id)

    own_rows = pltpu.make_async_copy(hidden, xg.at[pl.ds(0, r), :], hn_sem)
    own_rows.start()
    seg_copy = pltpu.make_async_copy(seg_hbm, seg, in_sem.at[0])
    freq_copy = pltpu.make_async_copy(freq_hbm, freq, in_sem.at[1])
    order_copy = pltpu.make_async_copy(order_hbm, order, in_sem.at[2])
    freq_copy.start()
    order_copy.start()
    seg_copy.start()
    wk_copy = pltpu.make_async_copy(wk, wb.at[:, pl.ds(Cq, Ck)], wkv_sem.at[0])
    wv_copy = pltpu.make_async_copy(wv, wb.at[:, pl.ds(Cq + Ck, Ck)], wkv_sem.at[1])
    wq_copy = pltpu.make_async_copy(wq, wb.at[:, pl.ds(0, Cq)], wq_sem)
    wo_copy = pltpu.make_async_copy(wo_hbm, wo, wo_sem)
    wk_copy.start()
    wv_copy.start()

    near = jnp.where(z > 0, 1, 0) + jnp.where(z < Z - 1, 1, 0)
    pl.semaphore_wait(barrier, 1 + (Y - 1) + (X - 1) + near)

    def tell(side, ok):
        @pl.when(ok)
        def _():
            pl.semaphore_signal(
                ready.at[side], inc=1, device_id=(s_id + (X if side == 0 else -X), h_id),
                device_id_type=MESH,
            )

    def hear(d):
        for side, there in ((0, z - d >= 0), (1, z + d < Z)):
            @pl.when(there)
            def _(side=side):
                pl.semaphore_wait(ready.at[side], 1)

            tell(side, there & ((z < Z - 1) if side == 0 else (z > 0)))

    tell(0, (z > 0) & (z < Z - 1))
    tell(1, (z < Z - 1) & (z > 0))

    def hid_pair():
        return pltpu.make_async_remote_copy(
            src_ref=xg.at[pl.ds(0, r), :], dst_ref=xg.at[pl.ds(r, r), :],
            send_sem=hs_sem, recv_sem=hp_sem,
            device_id=(s_id, partner), device_id_type=MESH,
        )

    def hid_send(j, e):
        return pltpu.make_async_remote_copy(
            src_ref=xg.at[pl.ds(e * part, part), :], dst_ref=xg.at[pl.ds(far_at(Y - j, e), part), :],
            send_sem=hs_sem, recv_sem=hd_sem.at[Y - j - 1, e],
            device_id=(s_id, peer_y(j) * CORES + c), device_id_type=MESH,
        )

    def hid_direct(j, e):
        rows = xg.at[pl.ds(far_at(j, e), part), :]
        return pltpu.make_async_remote_copy(
            src_ref=rows, dst_ref=rows, send_sem=hs_sem, recv_sem=hd_sem.at[j - 1, e],
            device_id=(s_id, partner), device_id_type=MESH,
        )

    def hid_relay(j, e):
        return pltpu.make_async_remote_copy(
            src_ref=xg.at[pl.ds(far_at(j, e), part), :],
            dst_ref=xg.at[pl.ds(far_at(j, e) + part, part), :],
            send_sem=hs_sem, recv_sem=hr_sem.at[j - 1, e],
            device_id=(s_id, partner), device_id_type=MESH,
        )

    own_rows.wait()
    hid_pair().start()
    for e in range(PARTS):
        for j in range(1, Y):
            hid_send(j, e).start()
    wq_copy.start()

    freq_copy.wait()
    order_copy.wait()
    for lo, n, first in runs:
        lane = lax.broadcasted_iota(jnp.int32, (n, HEAD_SIZE), 1)
        row = lax.broadcasted_iota(jnp.int32, (n, HEAD_SIZE), 0)
        angle = (row + place(s_id, first)).astype(F32) * freq[...]
        cos_t[lo:lo + n, :] = jnp.cos(angle)
        sn = jnp.sin(angle)
        sin_t[lo:lo + n, :] = jnp.where(lane < HEAD_SIZE // 2, -sn, sn)

    def kv_rows(zb, xb, lo, n):
        return kv.at[pl.ds((zb * X + xb) * R + lo, n), :]

    def col_copy(zb, p, target, sem):
        rows = kv_rows(zb, x, *pieces[p])
        return pltpu.make_async_remote_copy(
            src_ref=rows, dst_ref=rows, send_sem=sem, recv_sem=kc_sem.at[zb, p],
            device_id=(target, h_id), device_id_type=MESH,
        )

    def cross_copy(zb, xb, p, way, target, sem):
        rows = kv_rows(zb, xb, *pieces[p])
        return pltpu.make_async_remote_copy(
            src_ref=rows, dst_ref=rows, send_sem=sem, recv_sem=kx_sem.at[way - 1, zb, p],
            device_id=(target, h_id), device_id_type=MESH,
        )

    def send_x(zb, p):
        for k in range(1, X):
            cross_copy(zb, x, p, X - k, z * X + lax.rem(x + k, X), xs_sem).start()

    def send_up(zb, p):
        @pl.when(z < Z - 1)
        def _():
            col_copy(zb, p, s_id + X, zs_sem).start()

    def send_down(zb, p):
        @pl.when(z > 0)
        def _():
            col_copy(zb, p, s_id - X, zs_sem).start()

    def send_along(p, d):
        @pl.when(z + d < Z)
        def _():
            col_copy(z, p, s_id + d * X, zs_sem).start()

        @pl.when(z - d >= 0)
        def _():
            col_copy(z, p, s_id - d * X, zs_sem).start()

    def send_own(p):
        for d in range(1 if p < 2 else Z - 1, 0, -1):
            send_along(p, d)
        send_x(z, p)

    def at_end(a, b):
        return (a == 0) | (a == Z - 1) | (b == 0) | (b == Z - 1)

    def pass_on(d, p):
        for side, zb, there in ((0, z - d, z - d >= 0), (1, z + d, z + d < Z)):
            @pl.when(there)
            def _(side=side, zb=zb):
                col_copy(zb, p, s_id, zs_sem).wait_recv()
                if p < 2:
                    (send_up if side == 0 else send_down)(zb, p)
                if p < 2 or d > 1:
                    send_x(zb, p)
                else:
                    @pl.when(jnp.logical_not(at_end(z, zb)))
                    def _():
                        send_x(zb, p)

    def cross_wait(zb, way, p):
        cross_copy(zb, lax.rem(x + way, X), p, way, s_id, xs_sem).wait_recv()

    def cross_on(way, p):
        xb = lax.rem(x + way, X)
        cross_wait(z, way, p)

        @pl.when((z < Z - 1) & at_end(z, z + 1))
        def _():
            cross_copy(z, xb, p, way, s_id + X, zs_sem).start()

        @pl.when((z > 0) & at_end(z, z - 1))
        def _():
            cross_copy(z, xb, p, way, s_id - X, zs_sem).start()

    def store_kv(p):
        lo, n = pieces[p]
        got = jnp.dot(xg[lo:lo + n, :], wb[:, Cq:W], preferred_element_type=F32)
        turned = rotated(got[:, :Ck], cos_t[lo:lo + n, :], sin_t[lo:lo + n, :])
        rows = pl.ds(s_id * R + lo, n)
        for h in range(kv_heads):
            kv[rows, h * HEAD_SIZE:(h + 1) * HEAD_SIZE] = turned[h].astype(BF16)
        kv[rows, Ck:2 * Ck] = got[:, Ck:].astype(BF16)
        send_own(p)

    def store_q(u, side):
        lo, n = units[u]
        q = side[0]
        acc[0:n, :] = jnp.dot(xg[lo:lo + n, :], wb[:, :Cq], preferred_element_type=F32)
        turned = rotated(acc[0:n, :], cos_t[lo:lo + n, :], sin_t[lo:lo + n, :])
        for h in range(q_heads):
            at = (h % group) * n
            q[h // group, at:at + n, :] = turned[h].astype(BF16)

    wk_copy.wait()
    wv_copy.wait()
    store_kv(0)

    seg_copy.wait()
    starts = [
        jnp.sum(jnp.sum((seg[...] < v).astype(jnp.int32), axis=0, keepdims=True), axis=1, keepdims=True)
        for v in range(1, DOCS)
    ]
    for u, side in enumerate((near_side, far_side)):
        lo, n = units[u]
        info = side[5]
        for at, m, first in runs:
            if not lo <= at < lo + n:
                continue
            pos = lax.broadcasted_iota(jnp.int32, (1, m), 1) + place(s_id, first)
            start = jnp.zeros_like(pos)
            for begun in starts:
                start = jnp.where(begun <= pos, jnp.maximum(start, begun), start)
            for gh in range(info.shape[1] // n):
                lanes = slice(gh * n + at - lo, gh * n + at - lo + m)
                info[0:1, lanes] = pos
                info[1:2, lanes] = start
    for side in (far_side, near_side):
        side[1][...] = jnp.full_like(side[1], NEGATIVE_FILLER)
        side[2][...] = jnp.zeros_like(side[2])
        side[3][...] = jnp.zeros_like(side[3])

    hid_pair().wait_recv()
    store_kv(1)
    for d in range(2, min(3, Z)):
        hear(d)
    wo_copy.start()
    wq_copy.wait()
    store_q(0, near_side)

    scale = math.log2(math.e) / math.sqrt(HEAD_SIZE)
    nt = (((1,), (1,)), ((), ()))

    def nearest(n):
        low = jnp.minimum(z, Z - 1 - z)
        d = (n + 1) // 2
        both = jnp.where(lax.rem(n, 2) == 1, z - d, z + d)
        return jnp.where(n <= 2 * low, both, jnp.where(z < Z - 1 - z, n, Z - 1 - n))

    def attend(slots, u, side):
        q, m_s, l_s, o_s, bias, info = side
        chunk = bias.shape[1]
        lo, n = units[u]
        total = len(slots) * n
        for t, slot in enumerate(slots):
            for at, m, first in runs:
                if not lo <= at < lo + n:
                    continue
                kpos = lax.broadcasted_iota(jnp.int32, (m, chunk), 0) + place(slot, first)
                ok = (kpos <= info[0:1, :]) & (kpos >= info[1:2, :])
                bias[t * n + at - lo:t * n + at - lo + m, :] = jnp.where(ok, 0.0, NEGATIVE_FILLER)
        work = [(kh, w) for kh in range(kv_heads) for w in range(q.shape[1] // chunk)]
        span = lambda w: slice(w * chunk, (w + 1) * chunk)

        def gathered(col):
            cols = slice(col, col + HEAD_SIZE)
            return jnp.concatenate([kv[pl.ds(slot * R + lo, n), cols] for slot in slots], axis=0)

        keys = [gathered(kh * HEAD_SIZE) for kh in range(kv_heads)]
        vals = [gathered(Ck + kh * HEAD_SIZE).T for kh in range(kv_heads)]

        def scores(item):
            kh, w = item
            return lax.dot_general(keys[kh], q[kh, span(w), :], nt, preferred_element_type=F32)

        ahead = [scores(item) for item in work[:AHEAD]]
        for i, (kh, w) in enumerate(work):
            raw = ahead.pop(0)
            if i + AHEAD < len(work):
                ahead.append(scores(work[i + AHEAD]))
            cols = span(w)
            s = raw * scale + bias[0:total, :]
            old = m_s[kh:kh + 1, cols]
            new = jnp.maximum(old, jnp.max(s, axis=0, keepdims=True))
            p = jnp.exp2(s - new)
            alpha = jnp.exp2(old - new)
            m_s[kh:kh + 1, cols] = new
            l_s[kh:kh + 1, cols] = l_s[kh:kh + 1, cols] * alpha + jnp.sum(p, axis=0, keepdims=True)
            o_s[kh, :, cols] = o_s[kh, :, cols] * alpha + jnp.dot(
                vals[kh], p.astype(BF16), preferred_element_type=F32
            )

    def visit(u, side, first, last):
        def one(i, _):
            slots = []
            for t in range(TOGETHER):
                i_t = i * TOGETHER + t
                slots.append(nearest(lax.rem(i_t, Z)) * X + lax.rem(x + i_t // Z, X))
            attend(slots, u, side)
            return 0

        lax.fori_loop(first // TOGETHER, last // TOGETHER, one, 0)

    def settle(side, lo):
        q, m_s, l_s, o_s, bias, info = side
        wide = q.shape[1] // group
        for h in range(q_heads):
            kh, gh = h // group, h % group
            lanes = slice(gh * wide, (gh + 1) * wide)
            att[lo:lo + wide, h * HEAD_SIZE:(h + 1) * HEAD_SIZE] = (
                o_s[kh, :, lanes] / l_s[kh:kh + 1, lanes]
            ).T.astype(BF16)

    column, others = (0, 1), (1, X)


    def relay(first, last, p):
        for d in range(first, min(last, Z)):
            pass_on(d, p)

    def hidden_on(e):
        for j in range(1, Y):
            hid_direct(j, e).wait_recv()
            hid_relay(j, e).start()

    def hidden_in(e):
        for j in range(1, Y):
            hid_relay(j, e).wait_recv()

    def crossed(first, last, parts):
        for n in range(first, last):
            for way in range(1, X):
                for p in parts:
                    cross_wait(nearest(jnp.int32(n)), way, p)

    N_ALL, F_ALL = (0, 1), tuple(range(2, 2 + PARTS))
    last = PARTS - 1

    for d in range(3, Z):
        hear(d)
    relay(1, 2, 0)
    relay(1, 2, 1)
    for e in range(PARTS):
        if e == last:
            relay(2, 3, 0)
            relay(2, 3, 1)
        hidden_on(e)
        hidden_in(e)
        store_kv(2 + e)
    for p in F_ALL[:-1]:
        for way in range(1, X):
            cross_on(way, p)
    for d in range(Z - 1, 1, -1):
        for p in F_ALL[:-1]:
            relay(d, d + 1, p)
    store_q(1, far_side)
    for p in F_ALL[:-1]:
        relay(1, 2, p)
    relay(3, Z, 0)
    relay(3, Z, 1)
    for d in range(Z - 1, 1, -1):
        relay(d, d + 1, 1 + PARTS)
    for way in range(1, X):
        cross_on(way, 1 + PARTS)
    relay(1, 2, 1 + PARTS)
    visit(0, far_side, 0, Z)
    visit(1, far_side, 0, Z)
    crossed(0, Z, N_ALL)
    visit(0, far_side, Z, S)
    crossed(1, Z, F_ALL)
    visit(1, far_side, Z, S)
    settle(far_side, near_rows)
    wo_copy.wait()

    NW, PW = D // NO, D // NP

    def pair_far(j, n):
        cols = pl.ds(n * NW, NW)
        return pltpu.make_async_remote_copy(
            src_ref=give.at[j, :, cols], dst_ref=rb.at[j, :, cols],
            send_sem=ps_sem, recv_sem=pf_sem.at[j - 1, n],
            device_id=(s_id, partner), device_id_type=MESH,
        )

    def pair_near(n):
        cols = pl.ds(n * PW, PW)
        return pltpu.make_async_remote_copy(
            src_ref=give.at[0, :, cols], dst_ref=rb.at[0, :, cols],
            send_sem=ps_sem, recv_sem=pn_sem.at[n],
            device_id=(s_id, partner), device_id_type=MESH,
        )

    def far_copy(j, n):
        cols = pl.ds(n * NW, NW)
        return pltpu.make_async_remote_copy(
            src_ref=sb.at[j - 1, :, cols], dst_ref=fb.at[j - 1, :, cols],
            send_sem=ys_sem, recv_sem=yr_sem.at[j - 1, n],
            device_id=(s_id, peer_y(j) * CORES + c), device_id_type=MESH,
        )

    def project_far(n, _):
        @pl.when(n < NO)
        def _():
            cols = pl.ds(n * NW, NW)
            got = jnp.dot(att[near_rows:R, :], wo[:, cols], preferred_element_type=F32).astype(BF16)
            for j in range(1, Y):
                for e in range(PARTS):
                    at = far_at(j, e) - near_rows
                    keep[j, e * part:(e + 1) * part, cols] = got[at:at + part, :]
                    give[j, e * part:(e + 1) * part, cols] = got[at + part:at + 2 * part, :]
                pair_far(j, n).start()

        @pl.when(n >= LAG)
        def _():
            cols = pl.ds((n - LAG) * NW, NW)
            for j in range(1, Y):
                pair_far(j, n - LAG).wait_recv()
                sb[j - 1, :, cols] = (keep[j, :, cols].astype(F32) + rb[j, :, cols].astype(F32)).astype(BF16)
                far_copy(j, n - LAG).start()

        return 0

    lax.fori_loop(0, NO + LAG, project_far, 0)
    visit(0, near_side, 0, S)
    visit(1, near_side, 0, S)
    settle(near_side, 0)

    def project_near(n, _):
        cols = pl.ds(n * PW, PW)
        got = jnp.dot(att[0:near_rows, :], wo[:, cols], preferred_element_type=F32).astype(BF16)
        keep[0, :, cols] = got[:r, :]
        give[0, :, cols] = got[r:, :]
        pair_near(n).start()
        return 0

    lax.fori_loop(0, NP, project_near, 0)

    for n in range(NP):
        pair_near(n).wait_recv()

    def finish(n, _):
        cols = pl.ds(n * NW, NW)
        total = keep[0, :, cols].astype(F32) + rb[0, :, cols].astype(F32)
        for j in range(1, Y):
            far_copy(j, n).wait_recv()
            total = total + fb[j - 1, :, cols].astype(F32)
        out[:, cols] = total.astype(BF16)
        return 0

    lax.fori_loop(0, NO, finish, 0)

    def drain(ref, sem):
        pltpu.make_async_copy(ref, ref, sem).wait()

    drain(xg.at[pl.ds(0, (2 * Y - 1) * r), :], hs_sem)
    drain(give, ps_sem)
    drain(sb, ys_sem)
    for zz in range(Z):
        ends = (0, Z - 1)
        beside = [zb for zb in (zz - 1, zz + 1) if 0 <= zb < Z]
        bent = sum(zz in ends or zb in ends for zb in beside)
        early = (zz + 1) * (zz < Z - 1) + (Z - zz) * (zz > 0)
        along = early * near_rows + (Z - 1 + (X - 1) * bent) * far_rows
        over = (X - 1) * (Z * R - bent * far_rows)

        @pl.when(z == zz)
        def _(along=along, over=over):
            drain(kv.at[pl.ds(0, along), :], zs_sem)
            drain(kv.at[pl.ds(0, over), :], xs_sem)


def on_device(X, Z, Y, hidden, block_order, segment_ids, w_query, key_weight, value_weight, w_out):
    r, D = hidden.shape
    S, H = X * Z, Y * CORES
    R = r * H
    Cq, Ck = w_query.shape[1], key_weight.shape[1]
    W = Cq + 2 * Ck
    q_heads = Cq // HEAD_SIZE
    NO, NP = max(1, D // 512), max(1, D // 1024)
    PARTS = max(1, min(2, r // 16))
    exponent = np.arange(HEAD_SIZE // 2, dtype=np.float64) * 2.0 / HEAD_SIZE
    freqs = np.tile(ROPE_BASE ** (-exponent), 2).astype(np.float32)[None, :]
    dma = pltpu.SemaphoreType.DMA
    kv_heads = Ck // HEAD_SIZE
    group = q_heads // kv_heads
    near_rows, far_rows = CORES * r, R - CORES * r
    segments = segment_ids.reshape(block_order.shape[0], -1)

    def half_scratch(rows):
        together = 1 if rows % HEAD_SIZE == 0 else group
        lanes = group * rows
        return [
            pltpu.VMEM((kv_heads, lanes, HEAD_SIZE), BF16),
            pltpu.VMEM((kv_heads, lanes), F32),
            pltpu.VMEM((kv_heads, lanes), F32),
            pltpu.VMEM((kv_heads, HEAD_SIZE, lanes), F32),
            pltpu.VMEM((math.gcd(S, 4) * max(near_rows, far_rows), together * rows), F32),
            pltpu.VMEM((2, together * rows), jnp.int32),
        ]

    far = max(1, Y - 1)
    anywhere = pl.BlockSpec(memory_space=pl.ANY)
    return pl.pallas_call(
        functools.partial(kernel, X, Z, Y, PARTS, NO, NP),
        out_shape=pltpu.VMEM((r, D), BF16),
        in_specs=[anywhere] * 8,
        out_specs=pl.BlockSpec(memory_space=pltpu.VMEM),
        scratch_shapes=[
            pltpu.SMEM(block_order.shape, jnp.int32),
            pltpu.VMEM(segments.shape, jnp.int32),
            pltpu.VMEM((1, HEAD_SIZE), F32),
            pltpu.VMEM((R, D), BF16),
            pltpu.VMEM((D, W), BF16),
            pltpu.VMEM((Cq, D), BF16),
            pltpu.VMEM((max(near_rows, far_rows), Cq), F32),
            pltpu.VMEM((R, HEAD_SIZE), F32),
            pltpu.VMEM((R, HEAD_SIZE), F32),
            pltpu.VMEM((S * R, 2 * Ck), BF16),
            pltpu.VMEM((R, Cq), BF16),
            pltpu.VMEM((Y, r, D), BF16),
            pltpu.VMEM((Y, r, D), BF16),
            pltpu.VMEM((Y, r, D), BF16),
            pltpu.VMEM((far, r, D), BF16),
            pltpu.VMEM((far, r, D), BF16),
            *half_scratch(far_rows),
            *half_scratch(near_rows),
            dma((3,)), dma, dma((2,)), dma, dma,
            dma, dma, dma((far, PARTS)), dma((far, PARTS)),
            dma, dma, dma((Z, 2 + PARTS)), dma((max(1, X - 1), Z, 2 + PARTS)),
            dma, dma((far, NO)), dma((NP,)), dma, dma((far, NO)),
            pltpu.SemaphoreType.REGULAR((2,)),
        ],
        compiler_params=pltpu.CompilerParams(
            collective_id=0, has_side_effects=True, vmem_limit_bytes=60 * 1024 * 1024
        ),
    )(
        block_order, hidden, segments, jnp.asarray(freqs),
        w_query, key_weight, value_weight, w_out,
    )


def solution(mesh):
    seq, head = mesh.shape["seq"], mesh.shape["head"]
    X = 1
    while 4 * X * X <= seq and seq % (2 * X) == 0:
        X *= 2
    placed = (
        P(("seq", "head"), None),
        P(),
        P(),
        P(None, "head"),
        P(None, "head"),
        P(None, "head"),
        P("head", None),
    )
    return jax.shard_map(
        functools.partial(on_device, X, seq // X, head // CORES),
        mesh=mesh, in_specs=placed, out_specs=P(("seq", "head"), None), check_vma=False,
    )
```

```python
import functools
import math

import jax
import jax.numpy as jnp
import numpy as np
from jax import lax
from jax.experimental import pallas as pl
from jax.experimental.pallas import tpu as pltpu
from jax.sharding import PartitionSpec as P

HEAD_SIZE = 128
NEGATIVE_FILLER = -1e30
ROPE_BASE = 500000.0
DOCS = 4
CORES = 2
LAG = 3
AHEAD = 2
MESH = pl.DeviceIdType.MESH
F32 = jnp.float32
BF16 = jnp.bfloat16


def rotated(t, cosine, sine):
    heads = t.shape[1] // HEAD_SIZE
    pieces = []
    for h in range(heads):
        one = t[:, h * HEAD_SIZE:(h + 1) * HEAD_SIZE]
        pieces.append(one * cosine + pltpu.roll(one, HEAD_SIZE // 2, 1) * sine)
    return pieces


def kernel(
    X, Z, Y, PARTS, NO, NP,
    order_hbm, hidden, seg_hbm, freq_hbm, wq, wk, wv, wo_hbm, out,
    order, seg, freq, xg, wb, wo, acc, cos_t, sin_t, kv, att, keep, give, rb, sb, fb, *rest,
):
    far_side, near_side = rest[:6], rest[6:12]
    (in_sem, hn_sem, wkv_sem, wq_sem, wo_sem, hs_sem, hp_sem, hd_sem, hr_sem,
     xs_sem, zs_sem, kc_sem, kx_sem, ps_sem, pf_sem, pn_sem, ys_sem, yr_sem, ready) = rest[12:]
    r, D = hidden.shape
    R = xg.shape[0]
    Cq, Ck = wq.shape[1], wk.shape[1]
    half = R // 2
    q_heads, kv_heads = Cq // HEAD_SIZE, Ck // HEAD_SIZE
    group = q_heads // kv_heads
    W = Cq + 2 * Ck
    near_rows, far_rows = CORES * r, R - CORES * r
    part = r // PARTS
    wide_part = (Y - 1) * CORES * part
    S = X * Z
    TOGETHER = math.gcd(S, 4)
    s_id, h_id = lax.axis_index("seq"), lax.axis_index("head")
    y, c = h_id // CORES, h_id % CORES
    z, x = s_id // X, s_id % X
    partner = y * CORES + (1 - c)

    def peer_y(j):
        return lax.rem(y + j, Y)

    def far_at(j, e):
        return near_rows + e * wide_part + (j - 1) * CORES * part

    runs = [(0, r, h_id * r), (r, r, partner * r)]
    for e in range(PARTS):
        for j in range(1, Y):
            for i, core in enumerate((c, 1 - c)):
                runs.append((far_at(j, e) + i * part, part, (peer_y(j) * CORES + core) * r + e * part))
    pieces = [(0, r), (r, r)] + [(near_rows + e * wide_part, wide_part) for e in range(PARTS)]
    units = [(0, near_rows), (near_rows, far_rows)]

    def place(slot, first):
        return order[2 * slot + first // half] * half + lax.rem(first, half)

    barrier = pltpu.get_barrier_semaphore()

    def greet(sq, hd):
        pl.semaphore_signal(barrier, inc=1, device_id=(sq, hd), device_id_type=MESH)

    greet(s_id, partner)
    for j in range(1, Y):
        greet(s_id, peer_y(j) * CORES + c)
    for k in range(1, X):
        greet(z * X + lax.rem(x + k, X), h_id)

    @pl.when(z > 0)
    def _():
        greet(s_id - X, h_id)

    @pl.when(z < Z - 1)
    def _():
        greet(s_id + X, h_id)

    own_rows = pltpu.make_async_copy(hidden, xg.at[pl.ds(0, r), :], hn_sem)
    own_rows.start()
    seg_copy = pltpu.make_async_copy(seg_hbm, seg, in_sem.at[0])
    freq_copy = pltpu.make_async_copy(freq_hbm, freq, in_sem.at[1])
    order_copy = pltpu.make_async_copy(order_hbm, order, in_sem.at[2])
    freq_copy.start()
    order_copy.start()
    seg_copy.start()
    wk_copy = pltpu.make_async_copy(wk, wb.at[:, pl.ds(Cq, Ck)], wkv_sem.at[0])
    wv_copy = pltpu.make_async_copy(wv, wb.at[:, pl.ds(Cq + Ck, Ck)], wkv_sem.at[1])
    wq_copy = pltpu.make_async_copy(wq, wb.at[:, pl.ds(0, Cq)], wq_sem)
    wo_copy = pltpu.make_async_copy(wo_hbm, wo, wo_sem)
    wk_copy.start()
    wv_copy.start()

    near = jnp.where(z > 0, 1, 0) + jnp.where(z < Z - 1, 1, 0)
    pl.semaphore_wait(barrier, 1 + (Y - 1) + (X - 1) + near)

    def tell(side, ok):
        @pl.when(ok)
        def _():
            pl.semaphore_signal(
                ready.at[side], inc=1, device_id=(s_id + (X if side == 0 else -X), h_id),
                device_id_type=MESH,
            )

    def hear(d):
        for side, there in ((0, z - d >= 0), (1, z + d < Z)):
            @pl.when(there)
            def _(side=side):
                pl.semaphore_wait(ready.at[side], 1)

            tell(side, there & ((z < Z - 1) if side == 0 else (z > 0)))

    tell(0, (z > 0) & (z < Z - 1))
    tell(1, (z < Z - 1) & (z > 0))

    def hid_pair():
        return pltpu.make_async_remote_copy(
            src_ref=xg.at[pl.ds(0, r), :], dst_ref=xg.at[pl.ds(r, r), :],
            send_sem=hs_sem, recv_sem=hp_sem,
            device_id=(s_id, partner), device_id_type=MESH,
        )

    def hid_send(j, e):
        return pltpu.make_async_remote_copy(
            src_ref=xg.at[pl.ds(e * part, part), :], dst_ref=xg.at[pl.ds(far_at(Y - j, e), part), :],
            send_sem=hs_sem, recv_sem=hd_sem.at[Y - j - 1, e],
            device_id=(s_id, peer_y(j) * CORES + c), device_id_type=MESH,
        )

    def hid_direct(j, e):
        rows = xg.at[pl.ds(far_at(j, e), part), :]
        return pltpu.make_async_remote_copy(
            src_ref=rows, dst_ref=rows, send_sem=hs_sem, recv_sem=hd_sem.at[j - 1, e],
            device_id=(s_id, partner), device_id_type=MESH,
        )

    def hid_relay(j, e):
        return pltpu.make_async_remote_copy(
            src_ref=xg.at[pl.ds(far_at(j, e), part), :],
            dst_ref=xg.at[pl.ds(far_at(j, e) + part, part), :],
            send_sem=hs_sem, recv_sem=hr_sem.at[j - 1, e],
            device_id=(s_id, partner), device_id_type=MESH,
        )

    own_rows.wait()
    hid_pair().start()
    for e in range(PARTS):
        for j in range(1, Y):
            hid_send(j, e).start()
    wq_copy.start()

    freq_copy.wait()
    order_copy.wait()
    for lo, n, first in runs:
        lane = lax.broadcasted_iota(jnp.int32, (n, HEAD_SIZE), 1)
        row = lax.broadcasted_iota(jnp.int32, (n, HEAD_SIZE), 0)
        angle = (row + place(s_id, first)).astype(F32) * freq[...]
        cos_t[lo:lo + n, :] = jnp.cos(angle)
        sn = jnp.sin(angle)
        sin_t[lo:lo + n, :] = jnp.where(lane < HEAD_SIZE // 2, -sn, sn)

    def kv_rows(zb, xb, lo, n):
        return kv.at[pl.ds((zb * X + xb) * R + lo, n), :]

    def col_copy(zb, p, target, sem):
        rows = kv_rows(zb, x, *pieces[p])
        return pltpu.make_async_remote_copy(
            src_ref=rows, dst_ref=rows, send_sem=sem, recv_sem=kc_sem.at[zb, p],
            device_id=(target, h_id), device_id_type=MESH,
        )

    def cross_copy(zb, xb, p, way, target, sem):
        rows = kv_rows(zb, xb, *pieces[p])
        return pltpu.make_async_remote_copy(
            src_ref=rows, dst_ref=rows, send_sem=sem, recv_sem=kx_sem.at[way - 1, zb, p],
            device_id=(target, h_id), device_id_type=MESH,
        )

    def send_x(zb, p):
        for k in range(1, X):
            cross_copy(zb, x, p, X - k, z * X + lax.rem(x + k, X), xs_sem).start()

    def send_up(zb, p):
        @pl.when(z < Z - 1)
        def _():
            col_copy(zb, p, s_id + X, zs_sem).start()

    def send_down(zb, p):
        @pl.when(z > 0)
        def _():
            col_copy(zb, p, s_id - X, zs_sem).start()

    def send_along(p, d):
        @pl.when(z + d < Z)
        def _():
            col_copy(z, p, s_id + d * X, zs_sem).start()

        @pl.when(z - d >= 0)
        def _():
            col_copy(z, p, s_id - d * X, zs_sem).start()

    def send_own(p):
        for d in range(1 if p < 2 else Z - 1, 0, -1):
            send_along(p, d)
        send_x(z, p)

    def at_end(a, b):
        return (a == 0) | (a == Z - 1) | (b == 0) | (b == Z - 1)

    def pass_on(d, p):
        for side, zb, there in ((0, z - d, z - d >= 0), (1, z + d, z + d < Z)):
            @pl.when(there)
            def _(side=side, zb=zb):
                col_copy(zb, p, s_id, zs_sem).wait_recv()
                if p < 2:
                    (send_up if side == 0 else send_down)(zb, p)
                if p < 2 or d > 1:
                    send_x(zb, p)
                else:
                    @pl.when(jnp.logical_not(at_end(z, zb)))
                    def _():
                        send_x(zb, p)

    def cross_wait(zb, way, p):
        cross_copy(zb, lax.rem(x + way, X), p, way, s_id, xs_sem).wait_recv()

    def cross_on(way, p):
        xb = lax.rem(x + way, X)
        cross_wait(z, way, p)

        @pl.when((z < Z - 1) & at_end(z, z + 1))
        def _():
            cross_copy(z, xb, p, way, s_id + X, zs_sem).start()

        @pl.when((z > 0) & at_end(z, z - 1))
        def _():
            cross_copy(z, xb, p, way, s_id - X, zs_sem).start()

    def store_kv(p):
        lo, n = pieces[p]
        got = jnp.dot(xg[lo:lo + n, :], wb[:, Cq:W], preferred_element_type=F32)
        turned = rotated(got[:, :Ck], cos_t[lo:lo + n, :], sin_t[lo:lo + n, :])
        rows = pl.ds(s_id * R + lo, n)
        for h in range(kv_heads):
            kv[rows, h * HEAD_SIZE:(h + 1) * HEAD_SIZE] = turned[h].astype(BF16)
        kv[rows, Ck:2 * Ck] = got[:, Ck:].astype(BF16)
        send_own(p)

    def store_q(u, side):
        lo, n = units[u]
        q = side[0]
        acc[0:n, :] = jnp.dot(xg[lo:lo + n, :], wb[:, :Cq], preferred_element_type=F32)
        turned = rotated(acc[0:n, :], cos_t[lo:lo + n, :], sin_t[lo:lo + n, :])
        for h in range(q_heads):
            at = (h % group) * n
            q[h // group, at:at + n, :] = turned[h].astype(BF16)

    wk_copy.wait()
    wv_copy.wait()
    store_kv(0)

    seg_copy.wait()
    starts = [
        jnp.sum(jnp.sum((seg[...] < v).astype(jnp.int32), axis=0, keepdims=True), axis=1, keepdims=True)
        for v in range(1, DOCS)
    ]
    for u, side in enumerate((near_side, far_side)):
        lo, n = units[u]
        info = side[5]
        for at, m, first in runs:
            if not lo <= at < lo + n:
                continue
            pos = lax.broadcasted_iota(jnp.int32, (1, m), 1) + place(s_id, first)
            start = jnp.zeros_like(pos)
            for begun in starts:
                start = jnp.where(begun <= pos, jnp.maximum(start, begun), start)
            for gh in range(info.shape[1] // n):
                lanes = slice(gh * n + at - lo, gh * n + at - lo + m)
                info[0:1, lanes] = pos
                info[1:2, lanes] = start
    for side in (far_side, near_side):
        side[1][...] = jnp.full_like(side[1], NEGATIVE_FILLER)
        side[2][...] = jnp.zeros_like(side[2])
        side[3][...] = jnp.zeros_like(side[3])

    hid_pair().wait_recv()
    store_kv(1)
    for d in range(2, min(3, Z)):
        hear(d)
    wo_copy.start()
    wq_copy.wait()
    store_q(0, near_side)

    scale = math.log2(math.e) / math.sqrt(HEAD_SIZE)
    nt = (((1,), (1,)), ((), ()))

    def nearest(n):
        low = jnp.minimum(z, Z - 1 - z)
        d = (n + 1) // 2
        both = jnp.where(lax.rem(n, 2) == 1, z - d, z + d)
        return jnp.where(n <= 2 * low, both, jnp.where(z < Z - 1 - z, n, Z - 1 - n))

    def attend(slots, u, side):
        q, m_s, l_s, o_s, bias, info = side
        chunk = bias.shape[1]
        lo, n = units[u]
        total = len(slots) * n
        for t, slot in enumerate(slots):
            for at, m, first in runs:
                if not lo <= at < lo + n:
                    continue
                kpos = lax.broadcasted_iota(jnp.int32, (m, chunk), 0) + place(slot, first)
                ok = (kpos <= info[0:1, :]) & (kpos >= info[1:2, :])
                bias[t * n + at - lo:t * n + at - lo + m, :] = jnp.where(ok, 0.0, NEGATIVE_FILLER)
        work = [(kh, w) for kh in range(kv_heads) for w in range(q.shape[1] // chunk)]
        span = lambda w: slice(w * chunk, (w + 1) * chunk)

        def gathered(col):
            cols = slice(col, col + HEAD_SIZE)
            return jnp.concatenate([kv[pl.ds(slot * R + lo, n), cols] for slot in slots], axis=0)

        keys = [gathered(kh * HEAD_SIZE) for kh in range(kv_heads)]
        vals = [gathered(Ck + kh * HEAD_SIZE).T for kh in range(kv_heads)]

        def scores(item):
            kh, w = item
            return lax.dot_general(keys[kh], q[kh, span(w), :], nt, preferred_element_type=F32)

        ahead = [scores(item) for item in work[:AHEAD]]
        for i, (kh, w) in enumerate(work):
            raw = ahead.pop(0)
            if i + AHEAD < len(work):
                ahead.append(scores(work[i + AHEAD]))
            cols = span(w)
            s = raw * scale + bias[0:total, :]
            old = m_s[kh:kh + 1, cols]
            new = jnp.maximum(old, jnp.max(s, axis=0, keepdims=True))
            p = jnp.exp2(s - new)
            alpha = jnp.exp2(old - new)
            m_s[kh:kh + 1, cols] = new
            l_s[kh:kh + 1, cols] = l_s[kh:kh + 1, cols] * alpha + jnp.sum(p, axis=0, keepdims=True)
            o_s[kh, :, cols] = o_s[kh, :, cols] * alpha + jnp.dot(
                vals[kh], p.astype(BF16), preferred_element_type=F32
            )

    def visit(u, side, first, last):
        def one(i, _):
            slots = []
            for t in range(TOGETHER):
                i_t = i * TOGETHER + t
                slots.append(nearest(lax.rem(i_t, Z)) * X + lax.rem(x + i_t // Z, X))
            attend(slots, u, side)
            return 0

        lax.fori_loop(first // TOGETHER, last // TOGETHER, one, 0)

    def visit_these(u, side, pairs, count=TOGETHER):
        for first in range(0, len(pairs), count):
            attend(
                [nearest(jnp.int32(n)) * X + lax.rem(x + way, X) for n, way in pairs[first:first + count]],
                u, side,
            )

    def settle(side, lo):
        q, m_s, l_s, o_s, bias, info = side
        wide = q.shape[1] // group
        for h in range(q_heads):
            kh, gh = h // group, h % group
            lanes = slice(gh * wide, (gh + 1) * wide)
            att[lo:lo + wide, h * HEAD_SIZE:(h + 1) * HEAD_SIZE] = (
                o_s[kh, :, lanes] / l_s[kh:kh + 1, lanes]
            ).T.astype(BF16)

    column, others = (0, 1), (1, X)


    def relay(first, last, p):
        for d in range(first, min(last, Z)):
            pass_on(d, p)

    def hidden_on(e):
        for j in range(1, Y):
            hid_direct(j, e).wait_recv()
            hid_relay(j, e).start()

    def hidden_in(e):
        for j in range(1, Y):
            hid_relay(j, e).wait_recv()

    def crossed(first, last, parts):
        for n in range(first, last):
            for way in range(1, X):
                for p in parts:
                    cross_wait(nearest(jnp.int32(n)), way, p)

    N_ALL, F_ALL = (0, 1), tuple(range(2, 2 + PARTS))
    last = PARTS - 1

    for d in range(3, Z):
        hear(d)
    relay(1, 2, 0)
    relay(1, 2, 1)
    for e in range(PARTS):
        if e == last:
            relay(2, 3, 0)
            relay(2, 3, 1)
        hidden_on(e)
        hidden_in(e)
        store_kv(2 + e)
    for p in F_ALL[:-1]:
        for way in range(1, X):
            cross_on(way, p)
    for d in range(Z - 1, 1, -1):
        for p in F_ALL[:-1]:
            relay(d, d + 1, p)
    store_q(1, far_side)
    soon = [(n, 0) for n in range(min(3, Z))] + [(0, way) for way in range(1, X)]
    soon = soon[:len(soon) // TOGETHER * TOGETHER]
    later = [(n, way) for n in range(Z) for way in range(X) if (n, way) not in soon]
    crossed(0, 1, N_ALL)
    visit_these(0, far_side, soon)
    for p in F_ALL[:-1]:
        relay(1, 2, p)
    relay(3, Z, 0)
    relay(3, Z, 1)
    for d in range(Z - 1, 1, -1):
        relay(d, d + 1, 1 + PARTS)
    for way in range(1, X):
        cross_on(way, 1 + PARTS)
    relay(1, 2, 1 + PARTS)
    visit_these(1, far_side, [(n, 0) for n in range(Z)])
    crossed(1, Z, N_ALL)
    visit_these(0, far_side, later)
    half_far = [(n, way) for way in range(1, X) for n in (0, Z - 1)]
    rest_far = [(n, way) for way in range(1, X) for n in range(1, Z - 1)]
    crossed(Z - 1, Z, F_ALL)
    visit_these(1, far_side, half_far, max(1, TOGETHER // 2))
    crossed(1, Z - 1, F_ALL)
    visit_these(1, far_side, rest_far, max(1, TOGETHER // 2))
    settle(far_side, near_rows)
    wo_copy.wait()

    NW, PW = D // NO, D // NP

    def pair_far(j, n):
        cols = pl.ds(n * NW, NW)
        return pltpu.make_async_remote_copy(
            src_ref=give.at[j, :, cols], dst_ref=rb.at[j, :, cols],
            send_sem=ps_sem, recv_sem=pf_sem.at[j - 1, n],
            device_id=(s_id, partner), device_id_type=MESH,
        )

    def pair_near(n):
        cols = pl.ds(n * PW, PW)
        return pltpu.make_async_remote_copy(
            src_ref=give.at[0, :, cols], dst_ref=rb.at[0, :, cols],
            send_sem=ps_sem, recv_sem=pn_sem,
            device_id=(s_id, partner), device_id_type=MESH,
        )

    def far_copy(j, n):
        cols = pl.ds(n * NW, NW)
        return pltpu.make_async_remote_copy(
            src_ref=sb.at[j - 1, :, cols], dst_ref=fb.at[j - 1, :, cols],
            send_sem=ys_sem, recv_sem=yr_sem.at[j - 1, n // (NO - 1)],
            device_id=(s_id, peer_y(j) * CORES + c), device_id_type=MESH,
        )

    def project_far(n, _):
        @pl.when(n < NO)
        def _():
            cols = pl.ds(n * NW, NW)
            got = jnp.dot(att[near_rows:R, :], wo[:, cols], preferred_element_type=F32).astype(BF16)
            for j in range(1, Y):
                for e in range(PARTS):
                    at = far_at(j, e) - near_rows
                    keep[j, e * part:(e + 1) * part, cols] = got[at:at + part, :]
                    give[j, e * part:(e + 1) * part, cols] = got[at + part:at + 2 * part, :]
                pair_far(j, n).start()

        @pl.when(n >= LAG)
        def _():
            cols = pl.ds((n - LAG) * NW, NW)
            for j in range(1, Y):
                pair_far(j, n - LAG).wait_recv()
                sb[j - 1, :, cols] = (keep[j, :, cols].astype(F32) + rb[j, :, cols].astype(F32)).astype(BF16)
                far_copy(j, n - LAG).start()

        return 0

    lax.fori_loop(0, NO + LAG, project_far, 0)
    visit(0, near_side, 0, S)
    visit(1, near_side, 0, S)
    settle(near_side, 0)

    def project_near(n, _):
        cols = pl.ds(n * PW, PW)
        got = jnp.dot(att[0:near_rows, :], wo[:, cols], preferred_element_type=F32).astype(BF16)
        keep[0, :, cols] = got[:r, :]
        give[0, :, cols] = got[r:, :]
        pair_near(n).start()
        return 0

    lax.fori_loop(0, NP, project_near, 0)

    pltpu.make_async_copy(rb.at[0], rb.at[0], pn_sem).wait()

    def landed(j, n, count):
        rows = fb.at[j - 1, :, pl.ds(n * NW, count * NW)]
        pltpu.make_async_copy(rows, rows, yr_sem.at[j - 1, n // (NO - 1)]).wait()

    def finish(n, _):
        cols = pl.ds(n * NW, NW)
        total = keep[0, :, cols].astype(F32) + rb[0, :, cols].astype(F32)
        for j in range(1, Y):
            total = total + fb[j - 1, :, cols].astype(F32)
        out[:, cols] = total.astype(BF16)
        return 0

    for first, count in ((0, NO - 1), (NO - 1, 1)):
        for j in range(1, Y):
            landed(j, first, count)
        lax.fori_loop(first, first + count, finish, 0)

    def drain(ref, sem):
        pltpu.make_async_copy(ref, ref, sem).wait()

    drain(xg.at[pl.ds(0, (2 * Y - 1) * r), :], hs_sem)
    drain(give, ps_sem)
    drain(sb, ys_sem)
    for zz in range(Z):
        ends = (0, Z - 1)
        beside = [zb for zb in (zz - 1, zz + 1) if 0 <= zb < Z]
        bent = sum(zz in ends or zb in ends for zb in beside)
        early = (zz + 1) * (zz < Z - 1) + (Z - zz) * (zz > 0)
        along = early * near_rows + (Z - 1 + (X - 1) * bent) * far_rows
        over = (X - 1) * (Z * R - bent * far_rows)

        @pl.when(z == zz)
        def _(along=along, over=over):
            drain(kv.at[pl.ds(0, along), :], zs_sem)
            drain(kv.at[pl.ds(0, over), :], xs_sem)


def on_device(X, Z, Y, hidden, block_order, segment_ids, w_query, key_weight, value_weight, w_out):
    r, D = hidden.shape
    S, H = X * Z, Y * CORES
    R = r * H
    Cq, Ck = w_query.shape[1], key_weight.shape[1]
    W = Cq + 2 * Ck
    q_heads = Cq // HEAD_SIZE
    NO, NP = max(1, D // 512), max(1, D // 1024)
    PARTS = max(1, min(2, r // 16))
    exponent = np.arange(HEAD_SIZE // 2, dtype=np.float64) * 2.0 / HEAD_SIZE
    freqs = np.tile(ROPE_BASE ** (-exponent), 2).astype(np.float32)[None, :]
    dma = pltpu.SemaphoreType.DMA
    kv_heads = Ck // HEAD_SIZE
    group = q_heads // kv_heads
    near_rows, far_rows = CORES * r, R - CORES * r
    segments = segment_ids.reshape(block_order.shape[0], -1)

    def half_scratch(rows):
        together = 1 if rows % HEAD_SIZE == 0 else group
        lanes = group * rows
        return [
            pltpu.VMEM((kv_heads, lanes, HEAD_SIZE), BF16),
            pltpu.VMEM((kv_heads, lanes), F32),
            pltpu.VMEM((kv_heads, lanes), F32),
            pltpu.VMEM((kv_heads, HEAD_SIZE, lanes), F32),
            pltpu.VMEM((math.gcd(S, 4) * max(near_rows, far_rows), together * rows), F32),
            pltpu.VMEM((2, together * rows), jnp.int32),
        ]

    far = max(1, Y - 1)
    anywhere = pl.BlockSpec(memory_space=pl.ANY)
    return pl.pallas_call(
        functools.partial(kernel, X, Z, Y, PARTS, NO, NP),
        out_shape=pltpu.VMEM((r, D), BF16),
        in_specs=[anywhere] * 8,
        out_specs=pl.BlockSpec(memory_space=pltpu.VMEM),
        scratch_shapes=[
            pltpu.SMEM(block_order.shape, jnp.int32),
            pltpu.VMEM(segments.shape, jnp.int32),
            pltpu.VMEM((1, HEAD_SIZE), F32),
            pltpu.VMEM((R, D), BF16),
            pltpu.VMEM((D, W), BF16),
            pltpu.VMEM((Cq, D), BF16),
            pltpu.VMEM((max(near_rows, far_rows), Cq), F32),
            pltpu.VMEM((R, HEAD_SIZE), F32),
            pltpu.VMEM((R, HEAD_SIZE), F32),
            pltpu.VMEM((S * R, 2 * Ck), BF16),
            pltpu.VMEM((R, Cq), BF16),
            pltpu.VMEM((Y, r, D), BF16),
            pltpu.VMEM((Y, r, D), BF16),
            pltpu.VMEM((Y, r, D), BF16),
            pltpu.VMEM((far, r, D), BF16),
            pltpu.VMEM((far, r, D), BF16),
            *half_scratch(far_rows),
            *half_scratch(near_rows),
            dma((3,)), dma, dma((2,)), dma, dma,
            dma, dma, dma((far, PARTS)), dma((far, PARTS)),
            dma, dma, dma((Z, 2 + PARTS)), dma((max(1, X - 1), Z, 2 + PARTS)),
            dma, dma((far, NO)), dma, dma, dma((far, 2)),
            pltpu.SemaphoreType.REGULAR((2,)),
        ],
        compiler_params=pltpu.CompilerParams(
            collective_id=0, has_side_effects=True, vmem_limit_bytes=60 * 1024 * 1024
        ),
    )(
        block_order, hidden, segments, jnp.asarray(freqs),
        w_query, key_weight, value_weight, w_out,
    )


def solution(mesh):
    seq, head = mesh.shape["seq"], mesh.shape["head"]
    X = 1
    while 4 * X * X <= seq and seq % (2 * X) == 0:
        X *= 2
    placed = (
        P(("seq", "head"), None),
        P(),
        P(),
        P(None, "head"),
        P(None, "head"),
        P(None, "head"),
        P("head", None),
    )
    return jax.shard_map(
        functools.partial(on_device, X, seq // X, head // CORES),
        mesh=mesh, in_specs=placed, out_specs=P(("seq", "head"), None), check_vma=False,
    )
```

```python
import functools
import math

import jax
import jax.numpy as jnp
import numpy as np
from jax import lax
from jax.experimental import pallas as pl
from jax.experimental.pallas import tpu as pltpu
from jax.sharding import PartitionSpec as P

HEAD_SIZE = 128
NEGATIVE_FILLER = -1e30
ROPE_BASE = 500000.0
DOCS = 4
CORES = 2
LAG = 3
AHEAD = 2
MESH = pl.DeviceIdType.MESH
F32 = jnp.float32
BF16 = jnp.bfloat16


def rotated(t, cosine, sine):
    heads = t.shape[1] // HEAD_SIZE
    pieces = []
    for h in range(heads):
        one = t[:, h * HEAD_SIZE:(h + 1) * HEAD_SIZE]
        pieces.append(one * cosine + pltpu.roll(one, HEAD_SIZE // 2, 1) * sine)
    return pieces


def kernel(
    X, Z, Y, PARTS, NO, NP,
    order_hbm, hidden, seg_hbm, freq_hbm, wq, wk, wv, wo_hbm, out,
    order, seg, freq, xg, wb, wo, acc, cos_t, sin_t, kv, att, keep, give, rb, sb, fb, *rest,
):
    far_side, near_side = rest[:6], rest[6:12]
    (in_sem, hn_sem, wkv_sem, wq_sem, wo_sem, hs_sem, hp_sem, hd_sem, hr_sem,
     xs_sem, zs_sem, kc_sem, kx_sem, ps_sem, pf_sem, pn_sem, ys_sem, yr_sem, ready) = rest[12:]
    r, D = hidden.shape
    R = xg.shape[0]
    Cq, Ck = wq.shape[1], wk.shape[1]
    half = R // 2
    q_heads, kv_heads = Cq // HEAD_SIZE, Ck // HEAD_SIZE
    group = q_heads // kv_heads
    W = Cq + 2 * Ck
    near_rows, far_rows = CORES * r, R - CORES * r
    part = r // PARTS
    wide_part = (Y - 1) * CORES * part
    S = X * Z
    TOGETHER = math.gcd(S, 4)
    s_id, h_id = lax.axis_index("seq"), lax.axis_index("head")
    y, c = h_id // CORES, h_id % CORES
    z, x = s_id // X, s_id % X
    partner = y * CORES + (1 - c)

    def peer_y(j):
        return lax.rem(y + j, Y)

    def far_at(j, e):
        return near_rows + e * wide_part + (j - 1) * CORES * part

    runs = [(0, r, h_id * r), (r, r, partner * r)]
    for e in range(PARTS):
        for j in range(1, Y):
            for i, core in enumerate((c, 1 - c)):
                runs.append((far_at(j, e) + i * part, part, (peer_y(j) * CORES + core) * r + e * part))
    pieces = [(0, r), (r, r)] + [(near_rows + e * wide_part, wide_part) for e in range(PARTS)]
    units = [(0, near_rows), (near_rows, far_rows)]

    def place(slot, first):
        return order[2 * slot + first // half] * half + lax.rem(first, half)

    barrier = pltpu.get_barrier_semaphore()

    def greet(sq, hd):
        pl.semaphore_signal(barrier, inc=1, device_id=(sq, hd), device_id_type=MESH)

    greet(s_id, partner)
    for j in range(1, Y):
        greet(s_id, peer_y(j) * CORES + c)
    for k in range(1, X):
        greet(z * X + lax.rem(x + k, X), h_id)

    @pl.when(z > 0)
    def _():
        greet(s_id - X, h_id)

    @pl.when(z < Z - 1)
    def _():
        greet(s_id + X, h_id)

    own_rows = pltpu.make_async_copy(hidden, xg.at[pl.ds(0, r), :], hn_sem)
    own_rows.start()
    seg_copy = pltpu.make_async_copy(seg_hbm, seg, in_sem.at[0])
    freq_copy = pltpu.make_async_copy(freq_hbm, freq, in_sem.at[1])
    order_copy = pltpu.make_async_copy(order_hbm, order, in_sem.at[2])
    freq_copy.start()
    order_copy.start()
    seg_copy.start()
    wk_copy = pltpu.make_async_copy(wk, wb.at[:, pl.ds(Cq, Ck)], wkv_sem.at[0])
    wv_copy = pltpu.make_async_copy(wv, wb.at[:, pl.ds(Cq + Ck, Ck)], wkv_sem.at[1])
    wq_copy = pltpu.make_async_copy(wq, wb.at[:, pl.ds(0, Cq)], wq_sem)
    wo_copy = pltpu.make_async_copy(wo_hbm, wo, wo_sem)
    wk_copy.start()
    wv_copy.start()

    near = jnp.where(z > 0, 1, 0) + jnp.where(z < Z - 1, 1, 0)
    pl.semaphore_wait(barrier, 1 + (Y - 1) + (X - 1) + near)

    def tell(side, ok):
        @pl.when(ok)
        def _():
            pl.semaphore_signal(
                ready.at[side], inc=1, device_id=(s_id + (X if side == 0 else -X), h_id),
                device_id_type=MESH,
            )

    def hear(d):
        for side, there in ((0, z - d >= 0), (1, z + d < Z)):
            @pl.when(there)
            def _(side=side):
                pl.semaphore_wait(ready.at[side], 1)

            tell(side, there & ((z < Z - 1) if side == 0 else (z > 0)))

    tell(0, (z > 0) & (z < Z - 1))
    tell(1, (z < Z - 1) & (z > 0))

    def hid_pair():
        return pltpu.make_async_remote_copy(
            src_ref=xg.at[pl.ds(0, r), :], dst_ref=xg.at[pl.ds(r, r), :],
            send_sem=hs_sem, recv_sem=hp_sem,
            device_id=(s_id, partner), device_id_type=MESH,
        )

    def hid_send(j, e):
        return pltpu.make_async_remote_copy(
            src_ref=xg.at[pl.ds(e * part, part), :], dst_ref=xg.at[pl.ds(far_at(Y - j, e), part), :],
            send_sem=hs_sem, recv_sem=hd_sem.at[Y - j - 1, e],
            device_id=(s_id, peer_y(j) * CORES + c), device_id_type=MESH,
        )

    def hid_direct(j, e):
        rows = xg.at[pl.ds(far_at(j, e), part), :]
        return pltpu.make_async_remote_copy(
            src_ref=rows, dst_ref=rows, send_sem=hs_sem, recv_sem=hd_sem.at[j - 1, e],
            device_id=(s_id, partner), device_id_type=MESH,
        )

    def hid_relay(j, e):
        return pltpu.make_async_remote_copy(
            src_ref=xg.at[pl.ds(far_at(j, e), part), :],
            dst_ref=xg.at[pl.ds(far_at(j, e) + part, part), :],
            send_sem=hs_sem, recv_sem=hr_sem.at[j - 1, e],
            device_id=(s_id, partner), device_id_type=MESH,
        )

    own_rows.wait()
    hid_pair().start()
    for e in range(PARTS):
        for j in range(1, Y):
            hid_send(j, e).start()
    wq_copy.start()

    freq_copy.wait()
    order_copy.wait()
    for lo, n, first in runs:
        lane = lax.broadcasted_iota(jnp.int32, (n, HEAD_SIZE), 1)
        row = lax.broadcasted_iota(jnp.int32, (n, HEAD_SIZE), 0)
        angle = (row + place(s_id, first)).astype(F32) * freq[...]
        cos_t[lo:lo + n, :] = jnp.cos(angle)
        sn = jnp.sin(angle)
        sin_t[lo:lo + n, :] = jnp.where(lane < HEAD_SIZE // 2, -sn, sn)

    def kv_rows(zb, xb, lo, n):
        return kv.at[pl.ds((zb * X + xb) * R + lo, n), :]

    def col_copy(zb, p, target, sem):
        rows = kv_rows(zb, x, *pieces[p])
        return pltpu.make_async_remote_copy(
            src_ref=rows, dst_ref=rows, send_sem=sem, recv_sem=kc_sem.at[zb, p],
            device_id=(target, h_id), device_id_type=MESH,
        )

    def cross_copy(zb, xb, p, way, target, sem):
        rows = kv_rows(zb, xb, *pieces[p])
        return pltpu.make_async_remote_copy(
            src_ref=rows, dst_ref=rows, send_sem=sem, recv_sem=kx_sem.at[way - 1, zb, p],
            device_id=(target, h_id), device_id_type=MESH,
        )

    def send_x(zb, p):
        for k in range(1, X):
            cross_copy(zb, x, p, X - k, z * X + lax.rem(x + k, X), xs_sem).start()

    def send_up(zb, p):
        @pl.when(z < Z - 1)
        def _():
            col_copy(zb, p, s_id + X, zs_sem).start()

    def send_down(zb, p):
        @pl.when(z > 0)
        def _():
            col_copy(zb, p, s_id - X, zs_sem).start()

    def send_along(p, d):
        @pl.when(z + d < Z)
        def _():
            col_copy(z, p, s_id + d * X, zs_sem).start()

        @pl.when(z - d >= 0)
        def _():
            col_copy(z, p, s_id - d * X, zs_sem).start()

    def send_own(p):
        for d in range(1 if p < 2 else Z - 1, 0, -1):
            send_along(p, d)
        send_x(z, p)

    def at_end(a, b):
        return (a == 0) | (a == Z - 1) | (b == 0) | (b == Z - 1)

    def pass_on(d, p):
        for side, zb, there in ((0, z - d, z - d >= 0), (1, z + d, z + d < Z)):
            @pl.when(there)
            def _(side=side, zb=zb):
                col_copy(zb, p, s_id, zs_sem).wait_recv()
                if p < 2:
                    (send_up if side == 0 else send_down)(zb, p)
                if p < 2 or d > 1:
                    send_x(zb, p)
                else:
                    @pl.when(jnp.logical_not(at_end(z, zb)))
                    def _():
                        send_x(zb, p)

    def cross_wait(zb, way, p):
        cross_copy(zb, lax.rem(x + way, X), p, way, s_id, xs_sem).wait_recv()

    def cross_on(way, p):
        xb = lax.rem(x + way, X)
        cross_wait(z, way, p)

        @pl.when((z < Z - 1) & at_end(z, z + 1))
        def _():
            cross_copy(z, xb, p, way, s_id + X, zs_sem).start()

        @pl.when((z > 0) & at_end(z, z - 1))
        def _():
            cross_copy(z, xb, p, way, s_id - X, zs_sem).start()

    def store_kv(p):
        lo, n = pieces[p]
        got = jnp.dot(xg[lo:lo + n, :], wb[:, Cq:W], preferred_element_type=F32)
        turned = rotated(got[:, :Ck], cos_t[lo:lo + n, :], sin_t[lo:lo + n, :])
        rows = pl.ds(s_id * R + lo, n)
        for h in range(kv_heads):
            kv[rows, h * HEAD_SIZE:(h + 1) * HEAD_SIZE] = turned[h].astype(BF16)
        kv[rows, Ck:2 * Ck] = got[:, Ck:].astype(BF16)
        send_own(p)

    def store_q(u, side):
        lo, n = units[u]
        q = side[0]
        acc[0:n, :] = jnp.dot(xg[lo:lo + n, :], wb[:, :Cq], preferred_element_type=F32)
        turned = rotated(acc[0:n, :], cos_t[lo:lo + n, :], sin_t[lo:lo + n, :])
        for h in range(q_heads):
            at = (h % group) * n
            q[h // group, at:at + n, :] = turned[h].astype(BF16)

    wk_copy.wait()
    wv_copy.wait()
    store_kv(0)

    seg_copy.wait()
    starts = [
        jnp.sum(jnp.sum((seg[...] < v).astype(jnp.int32), axis=0, keepdims=True), axis=1, keepdims=True)
        for v in range(1, DOCS)
    ]
    for u, side in enumerate((near_side, far_side)):
        lo, n = units[u]
        info = side[5]
        for at, m, first in runs:
            if not lo <= at < lo + n:
                continue
            pos = lax.broadcasted_iota(jnp.int32, (1, m), 1) + place(s_id, first)
            start = jnp.zeros_like(pos)
            for begun in starts:
                start = jnp.where(begun <= pos, jnp.maximum(start, begun), start)
            for gh in range(info.shape[1] // n):
                lanes = slice(gh * n + at - lo, gh * n + at - lo + m)
                info[0:1, lanes] = pos
                info[1:2, lanes] = start
    for side in (far_side, near_side):
        side[1][...] = jnp.full_like(side[1], NEGATIVE_FILLER)
        side[2][...] = jnp.zeros_like(side[2])
        side[3][...] = jnp.zeros_like(side[3])

    hid_pair().wait_recv()
    store_kv(1)
    for d in range(2, min(3, Z)):
        hear(d)
    wo_copy.start()
    wq_copy.wait()
    store_q(0, near_side)

    scale = math.log2(math.e) / math.sqrt(HEAD_SIZE)
    nt = (((1,), (1,)), ((), ()))

    def nearest(n):
        low = jnp.minimum(z, Z - 1 - z)
        d = (n + 1) // 2
        both = jnp.where(lax.rem(n, 2) == 1, z - d, z + d)
        return jnp.where(n <= 2 * low, both, jnp.where(z < Z - 1 - z, n, Z - 1 - n))

    def attend(slots, u, side):
        q, m_s, l_s, o_s, bias, info = side
        chunk = bias.shape[1]
        lo, n = units[u]
        total = len(slots) * n
        for t, slot in enumerate(slots):
            for at, m, first in runs:
                if not lo <= at < lo + n:
                    continue
                kpos = lax.broadcasted_iota(jnp.int32, (m, chunk), 0) + place(slot, first)
                ok = (kpos <= info[0:1, :]) & (kpos >= info[1:2, :])
                bias[t * n + at - lo:t * n + at - lo + m, :] = jnp.where(ok, 0.0, NEGATIVE_FILLER)
        work = [(kh, w) for kh in range(kv_heads) for w in range(q.shape[1] // chunk)]
        span = lambda w: slice(w * chunk, (w + 1) * chunk)

        def gathered(col):
            cols = slice(col, col + HEAD_SIZE)
            return jnp.concatenate([kv[pl.ds(slot * R + lo, n), cols] for slot in slots], axis=0)

        keys = [gathered(kh * HEAD_SIZE) for kh in range(kv_heads)]
        vals = [gathered(Ck + kh * HEAD_SIZE).T for kh in range(kv_heads)]

        def scores(item):
            kh, w = item
            return lax.dot_general(keys[kh], q[kh, span(w), :], nt, preferred_element_type=F32)

        ahead = [scores(item) for item in work[:AHEAD]]
        for i, (kh, w) in enumerate(work):
            raw = ahead.pop(0)
            if i + AHEAD < len(work):
                ahead.append(scores(work[i + AHEAD]))
            cols = span(w)
            s = raw * scale + bias[0:total, :]
            old = m_s[kh:kh + 1, cols]
            new = jnp.maximum(old, jnp.max(s, axis=0, keepdims=True))
            p = jnp.exp2(s - new)
            alpha = jnp.exp2(old - new)
            m_s[kh:kh + 1, cols] = new
            l_s[kh:kh + 1, cols] = l_s[kh:kh + 1, cols] * alpha + jnp.sum(p, axis=0, keepdims=True)
            o_s[kh, :, cols] = o_s[kh, :, cols] * alpha + jnp.dot(
                vals[kh], p.astype(BF16), preferred_element_type=F32
            )

    def visit(u, side, first, last):
        def one(i, _):
            slots = []
            for t in range(TOGETHER):
                i_t = i * TOGETHER + t
                slots.append(nearest(lax.rem(i_t, Z)) * X + lax.rem(x + i_t // Z, X))
            attend(slots, u, side)
            return 0

        lax.fori_loop(first // TOGETHER, last // TOGETHER, one, 0)

    def visit_these(u, side, pairs, count=TOGETHER):
        for first in range(0, len(pairs), count):
            attend(
                [nearest(jnp.int32(n)) * X + lax.rem(x + way, X) for n, way in pairs[first:first + count]],
                u, side,
            )

    def settle(side, lo):
        q, m_s, l_s, o_s, bias, info = side
        wide = q.shape[1] // group
        for h in range(q_heads):
            kh, gh = h // group, h % group
            lanes = slice(gh * wide, (gh + 1) * wide)
            att[lo:lo + wide, h * HEAD_SIZE:(h + 1) * HEAD_SIZE] = (
                o_s[kh, :, lanes] / l_s[kh:kh + 1, lanes]
            ).T.astype(BF16)

    column, others = (0, 1), (1, X)


    def relay(first, last, p):
        for d in range(first, min(last, Z)):
            pass_on(d, p)

    def hidden_on(e):
        for j in range(1, Y):
            hid_direct(j, e).wait_recv()
            hid_relay(j, e).start()

    def hidden_in(e):
        for j in range(1, Y):
            hid_relay(j, e).wait_recv()

    def crossed(first, last, parts):
        for n in range(first, last):
            for way in range(1, X):
                for p in parts:
                    cross_wait(nearest(jnp.int32(n)), way, p)

    N_ALL, F_ALL = (0, 1), tuple(range(2, 2 + PARTS))
    last = PARTS - 1

    for d in range(3, Z):
        hear(d)
    relay(1, 2, 0)
    relay(1, 2, 1)
    for e in range(PARTS):
        if e == last:
            relay(2, 3, 0)
            relay(2, 3, 1)
        hidden_on(e)
        hidden_in(e)
        store_kv(2 + e)
    for d in range(Z - 1, 1, -1):
        for p in F_ALL[:-1]:
            relay(d, d + 1, p)
    store_q(1, far_side)
    soon = [(n, 0) for n in range(min(3, Z))] + [(0, way) for way in range(1, X)]
    soon = soon[:len(soon) // TOGETHER * TOGETHER]
    later = [(n, way) for n in range(Z) for way in range(X) if (n, way) not in soon]
    crossed(0, 1, N_ALL)
    visit_these(0, far_side, soon)
    for p in F_ALL[:-1]:
        relay(1, 2, p)
    relay(3, Z, 0)
    relay(3, Z, 1)
    for d in range(Z - 1, 1, -1):
        relay(d, d + 1, 1 + PARTS)
    for p in F_ALL[:-1]:
        for way in range(1, X):
            cross_on(way, p)
    for way in range(1, X):
        cross_on(way, 1 + PARTS)
    relay(1, 2, 1 + PARTS)
    visit_these(1, far_side, [(n, 0) for n in range(Z)])
    crossed(1, Z, N_ALL)
    visit_these(0, far_side, later)
    half_far = [(n, way) for way in range(1, X) for n in (0, Z - 1)]
    rest_far = [(n, way) for way in range(1, X) for n in range(1, Z - 1)]
    crossed(Z - 1, Z, F_ALL)
    visit_these(1, far_side, half_far, max(1, TOGETHER // 2))
    crossed(1, Z - 1, F_ALL)
    visit_these(1, far_side, rest_far, max(1, TOGETHER // 2))
    settle(far_side, near_rows)
    wo_copy.wait()

    NW, PW = D // NO, D // NP

    def pair_far(j, n):
        cols = pl.ds(n * NW, NW)
        return pltpu.make_async_remote_copy(
            src_ref=give.at[j, :, cols], dst_ref=rb.at[j, :, cols],
            send_sem=ps_sem, recv_sem=pf_sem.at[j - 1, n],
            device_id=(s_id, partner), device_id_type=MESH,
        )

    def pair_near(n):
        cols = pl.ds(n * PW, PW)
        return pltpu.make_async_remote_copy(
            src_ref=give.at[0, :, cols], dst_ref=rb.at[0, :, cols],
            send_sem=ps_sem, recv_sem=pn_sem,
            device_id=(s_id, partner), device_id_type=MESH,
        )

    def far_copy(j, n):
        cols = pl.ds(n * NW, NW)
        return pltpu.make_async_remote_copy(
            src_ref=sb.at[j - 1, :, cols], dst_ref=fb.at[j - 1, :, cols],
            send_sem=ys_sem, recv_sem=yr_sem.at[j - 1, n // (NO - 1)],
            device_id=(s_id, peer_y(j) * CORES + c), device_id_type=MESH,
        )

    def project_far(n, _):
        @pl.when(n < NO)
        def _():
            cols = pl.ds(n * NW, NW)
            got = jnp.dot(att[near_rows:R, :], wo[:, cols], preferred_element_type=F32).astype(BF16)
            for j in range(1, Y):
                for e in range(PARTS):
                    at = far_at(j, e) - near_rows
                    keep[j, e * part:(e + 1) * part, cols] = got[at:at + part, :]
                    give[j, e * part:(e + 1) * part, cols] = got[at + part:at + 2 * part, :]
                pair_far(j, n).start()

        @pl.when(n >= LAG)
        def _():
            cols = pl.ds((n - LAG) * NW, NW)
            for j in range(1, Y):
                pair_far(j, n - LAG).wait_recv()
                sb[j - 1, :, cols] = (keep[j, :, cols].astype(F32) + rb[j, :, cols].astype(F32)).astype(BF16)
                far_copy(j, n - LAG).start()

        return 0

    lax.fori_loop(0, NO + LAG, project_far, 0)
    visit(0, near_side, 0, S)
    visit(1, near_side, 0, S)
    settle(near_side, 0)

    def project_near(n, _):
        cols = pl.ds(n * PW, PW)
        got = jnp.dot(att[0:near_rows, :], wo[:, cols], preferred_element_type=F32).astype(BF16)
        keep[0, :, cols] = got[:r, :]
        give[0, :, cols] = got[r:, :]
        pair_near(n).start()
        return 0

    lax.fori_loop(0, NP, project_near, 0)

    pltpu.make_async_copy(rb.at[0], rb.at[0], pn_sem).wait()

    def landed(j, n, count):
        rows = fb.at[j - 1, :, pl.ds(n * NW, count * NW)]
        pltpu.make_async_copy(rows, rows, yr_sem.at[j - 1, n // (NO - 1)]).wait()

    def finish(n, _):
        cols = pl.ds(n * NW, NW)
        total = keep[0, :, cols].astype(F32) + rb[0, :, cols].astype(F32)
        for j in range(1, Y):
            total = total + fb[j - 1, :, cols].astype(F32)
        out[:, cols] = total.astype(BF16)
        return 0

    for first, count in ((0, NO - 1), (NO - 1, 1)):
        for j in range(1, Y):
            landed(j, first, count)
        lax.fori_loop(first, first + count, finish, 0)

    def drain(ref, sem):
        pltpu.make_async_copy(ref, ref, sem).wait()

    drain(xg.at[pl.ds(0, (2 * Y - 1) * r), :], hs_sem)
    drain(give, ps_sem)
    drain(sb, ys_sem)
    for zz in range(Z):
        ends = (0, Z - 1)
        beside = [zb for zb in (zz - 1, zz + 1) if 0 <= zb < Z]
        bent = sum(zz in ends or zb in ends for zb in beside)
        early = (zz + 1) * (zz < Z - 1) + (Z - zz) * (zz > 0)
        along = early * near_rows + (Z - 1 + (X - 1) * bent) * far_rows
        over = (X - 1) * (Z * R - bent * far_rows)

        @pl.when(z == zz)
        def _(along=along, over=over):
            drain(kv.at[pl.ds(0, along), :], zs_sem)
            drain(kv.at[pl.ds(0, over), :], xs_sem)


def on_device(X, Z, Y, hidden, block_order, segment_ids, w_query, key_weight, value_weight, w_out):
    r, D = hidden.shape
    S, H = X * Z, Y * CORES
    R = r * H
    Cq, Ck = w_query.shape[1], key_weight.shape[1]
    W = Cq + 2 * Ck
    q_heads = Cq // HEAD_SIZE
    NO, NP = max(1, D // 512), max(1, D // 1024)
    PARTS = max(1, min(2, r // 16))
    exponent = np.arange(HEAD_SIZE // 2, dtype=np.float64) * 2.0 / HEAD_SIZE
    freqs = np.tile(ROPE_BASE ** (-exponent), 2).astype(np.float32)[None, :]
    dma = pltpu.SemaphoreType.DMA
    kv_heads = Ck // HEAD_SIZE
    group = q_heads // kv_heads
    near_rows, far_rows = CORES * r, R - CORES * r
    segments = segment_ids.reshape(block_order.shape[0], -1)

    def half_scratch(rows):
        together = 1 if rows % HEAD_SIZE == 0 else group
        lanes = group * rows
        return [
            pltpu.VMEM((kv_heads, lanes, HEAD_SIZE), BF16),
            pltpu.VMEM((kv_heads, lanes), F32),
            pltpu.VMEM((kv_heads, lanes), F32),
            pltpu.VMEM((kv_heads, HEAD_SIZE, lanes), F32),
            pltpu.VMEM((math.gcd(S, 4) * max(near_rows, far_rows), together * rows), F32),
            pltpu.VMEM((2, together * rows), jnp.int32),
        ]

    far = max(1, Y - 1)
    anywhere = pl.BlockSpec(memory_space=pl.ANY)
    return pl.pallas_call(
        functools.partial(kernel, X, Z, Y, PARTS, NO, NP),
        out_shape=pltpu.VMEM((r, D), BF16),
        in_specs=[anywhere] * 8,
        out_specs=pl.BlockSpec(memory_space=pltpu.VMEM),
        scratch_shapes=[
            pltpu.SMEM(block_order.shape, jnp.int32),
            pltpu.VMEM(segments.shape, jnp.int32),
            pltpu.VMEM((1, HEAD_SIZE), F32),
            pltpu.VMEM((R, D), BF16),
            pltpu.VMEM((D, W), BF16),
            pltpu.VMEM((Cq, D), BF16),
            pltpu.VMEM((max(near_rows, far_rows), Cq), F32),
            pltpu.VMEM((R, HEAD_SIZE), F32),
            pltpu.VMEM((R, HEAD_SIZE), F32),
            pltpu.VMEM((S * R, 2 * Ck), BF16),
            pltpu.VMEM((R, Cq), BF16),
            pltpu.VMEM((Y, r, D), BF16),
            pltpu.VMEM((Y, r, D), BF16),
            pltpu.VMEM((Y, r, D), BF16),
            pltpu.VMEM((far, r, D), BF16),
            pltpu.VMEM((far, r, D), BF16),
            *half_scratch(far_rows),
            *half_scratch(near_rows),
            dma((3,)), dma, dma((2,)), dma, dma,
            dma, dma, dma((far, PARTS)), dma((far, PARTS)),
            dma, dma, dma((Z, 2 + PARTS)), dma((max(1, X - 1), Z, 2 + PARTS)),
            dma, dma((far, NO)), dma, dma, dma((far, 2)),
            pltpu.SemaphoreType.REGULAR((2,)),
        ],
        compiler_params=pltpu.CompilerParams(
            collective_id=0, has_side_effects=True, vmem_limit_bytes=60 * 1024 * 1024
        ),
    )(
        block_order, hidden, segments, jnp.asarray(freqs),
        w_query, key_weight, value_weight, w_out,
    )


def solution(mesh):
    seq, head = mesh.shape["seq"], mesh.shape["head"]
    X = 1
    while 4 * X * X <= seq and seq % (2 * X) == 0:
        X *= 2
    placed = (
        P(("seq", "head"), None),
        P(),
        P(),
        P(None, "head"),
        P(None, "head"),
        P(None, "head"),
        P("head", None),
    )
    return jax.shard_map(
        functools.partial(on_device, X, seq // X, head // CORES),
        mesh=mesh, in_specs=placed, out_specs=P(("seq", "head"), None), check_vma=False,
    )
```
